8 devices in a mesh: vp: 8 (over z, y, x, core).
Axes of the slice: x: 2, y: 2, z: 1, core: 2. Of those that a mesh axis runs over, the one named last changes fastest.
Arguments:
- hidden: bfloat16 [128, 1536], replicated
- ln_weight: bfloat16 [1536], replicated
- ln_bias: bfloat16 [1536], replicated
- embedding: bfloat16 [250880, 1536], P('vp')
- temperature: float32 [], replicated
- cand_ids: int32 [128, 128], replicated
Outputs:
- output 1: float32 [128, 250880], P(None, 'vp')
- output 2: float32 [128, 128], replicated
All inputs are finite; a program needn't handle non-finite values.
Results may differ from the reference program's by a relative error of at most 0.001.
Values sent between devices are 32-bit elements.
A program may use at most 1 GiB of HBM per device.

```python
import jax
import jax.numpy as jnp
from jax import lax

BATCH = 128
HIDDEN = 1536
VOCAB = 250880
CANDS = 128
CLUSTER_IDS = VOCAB // 64


def hot_scales(key_rows):
    hot_draw = jax.random.randint(key_rows, (VOCAB,), 0, 64)
    return jnp.where(hot_draw == 0, 3.0, 1.0).astype(jnp.float32)


def draw_candidates(key_cand):
    k_center, k_pick, k_offset, k_spread = jax.random.split(key_cand, 4)
    centers = jax.random.randint(k_center, (3,), 0, VOCAB - CLUSTER_IDS)
    pick_idx = jax.random.randint(k_pick, (BATCH, CANDS), 0, 3)
    offsets = jax.random.randint(k_offset, (BATCH, CANDS), 0, CLUSTER_IDS)
    spread = jax.random.randint(k_spread, (BATCH, CANDS), 0, VOCAB)
    clustered = jnp.take(centers, pick_idx) + offsets
    column = jnp.arange(CANDS)[None, :]
    cand_ids = jnp.where(column % 4 == 3, spread, clustered)
    cand_ids = cand_ids.at[0, 0].set(0).at[BATCH - 1, CANDS - 1].set(VOCAB - 1)
    return cand_ids.astype(jnp.int32)


def setup_inputs(seed: int = 0) -> dict:
    root_key = jax.random.key(seed)
    k_hidden, k_weight, k_bias, k_embed, k_hot, k_temp, k_cand = jax.random.split(root_key, 7)
    hidden = jax.random.normal(k_hidden, (BATCH, HIDDEN), jnp.float32)
    ln_weight = 1.0 + 0.5 * jax.random.normal(k_weight, (HIDDEN,), jnp.float32)
    ln_bias = 0.5 * jax.random.normal(k_bias, (HIDDEN,), jnp.float32)
    row_gain = hot_scales(k_hot) * (HIDDEN ** -0.5)
    embedding = jax.random.normal(k_embed, (VOCAB, HIDDEN), jnp.float32) * row_gain[:, None]
    temperature = jax.random.uniform(k_temp, (), jnp.float32, minval=0.8, maxval=1.25)
    return {
        "hidden": hidden.astype(jnp.bfloat16),
        "ln_weight": ln_weight.astype(jnp.bfloat16),
        "ln_bias": ln_bias.astype(jnp.bfloat16),
        "embedding": embedding.astype(jnp.bfloat16),
        "temperature": temperature,
        "cand_ids": draw_candidates(k_cand),
    }


def reference(hidden, ln_weight, ln_bias, embedding, temperature, cand_ids):
    hidden_f32 = hidden.astype(jnp.float32)
    row_mean = jnp.mean(hidden_f32, axis=-1, keepdims=True)
    centered = hidden_f32 - row_mean
    row_var = jnp.mean(centered * centered, axis=-1, keepdims=True)
    scaled = centered * lax.rsqrt(row_var + 1e-5)
    normed = (scaled * ln_weight.astype(jnp.float32) + ln_bias.astype(jnp.float32)).astype(jnp.bfloat16)
    logits = lax.dot_general(normed, embedding, (((1,), (1,)), ((), ())), preferred_element_type=jnp.float32) / temperature
    row_max = jnp.max(logits, axis=1, keepdims=True)
    exp_sum = jnp.sum(jnp.exp(logits - row_max), axis=1, keepdims=True)
    logprobs = logits - (row_max + jnp.log(exp_sum))
    cand_lp = jnp.take_along_axis(logprobs, cand_ids, axis=1)
    return logprobs, cand_lp
```

```python
import functools

import jax
import jax.numpy as jnp
from jax import lax
from jax.experimental import pallas as pl
from jax.experimental.pallas import tpu as pltpu
from jax.sharding import PartitionSpec as P

MESH_ID = pl.DeviceIdType.MESH
LANES = 128
TILE = 1792
DEPTH = 4


def split_columns(columns, tile):
    full = columns // tile
    return full, columns - full * tile


def head_kernel(
    axis_name, n_dev, tile, full, rest,
    temp_ref, x_ref, w_ref, b_ref, cand_ref, emb_ref,
    z_ref, logz_ref, q_ref,
    ebuf, raw_a, raw_b, normed, m_ref, l_ref, cand_hi, cand_lo, q_part,
    stat_send, stat_recv, qrs_recv, q_own, q_all,
    e_sem, stat_ssem, stat_rsem, rs_ssem, rs_rsem, ag_ssem, ag_rsem,
):
    me = lax.axis_index(axis_name)
    rows, _ = x_ref.shape
    columns = emb_ref.shape[0]
    depth = ebuf.shape[0]
    groups = rows // 8
    own_rows = rows // n_dev

    def load(t, slot):
        return pltpu.make_async_copy(
            emb_ref.at[pl.ds(pl.multiple_of(t * tile, LANES), tile)], ebuf.at[slot], e_sem.at[slot])

    def load_rest(slot):
        return pltpu.make_async_copy(
            emb_ref.at[pl.ds(full * tile, rest)], ebuf.at[slot, pl.ds(0, rest)], e_sem.at[slot])

    def start_any(t):
        if t < full:
            load(t, t % depth).start()
        elif t == full and rest:
            load_rest(t % depth).start()

    barrier = pltpu.get_barrier_semaphore()
    for k in range(1, n_dev):
        pl.semaphore_signal(barrier, inc=1, device_id=(lax.rem(me + k, n_dev),), device_id_type=MESH_ID)
    for t in range(depth - 1):
        start_any(t)

    xf = x_ref[...].astype(jnp.float32)
    mean = jnp.mean(xf, axis=-1, keepdims=True)
    cent = xf - mean
    var = jnp.mean(cent * cent, axis=-1, keepdims=True)
    scaled = cent * lax.rsqrt(var + 1e-5)
    normed[...] = (scaled * w_ref[...].astype(jnp.float32) + b_ref[...].astype(jnp.float32)).astype(jnp.bfloat16)
    local = cand_ref[...] - me * columns
    cand_hi[...] = local >> 7
    cand_lo[...] = local & (LANES - 1)
    m_ref[...] = jnp.full_like(m_ref, -jnp.inf)
    l_ref[...] = jnp.zeros_like(l_ref)
    q_part[...] = jnp.zeros_like(q_part)
    inv_t = 1.0 / jnp.full((8, LANES), temp_ref[0, 0], jnp.float32)

    def dot(slot, raw, width):
        raw[:, :width] = lax.dot_general(
            normed[...], ebuf[slot, :width], (((1,), (1,)), ((), ())), preferred_element_type=jnp.float32)

    def epilogue(t, raw, width):
        for g in range(groups):
            r = pl.ds(8 * g, 8)
            zs = []
            for j in range(width // LANES):
                z = raw[r, j * LANES:(j + 1) * LANES] * inv_t
                z_ref[r, pl.ds(pl.multiple_of(t * tile + j * LANES, LANES), LANES)] = z
                zs.append(z)
            top = functools.reduce(jnp.maximum, zs)
            m_old = m_ref[r, :]
            m_new = jnp.maximum(m_old, top)
            total = l_ref[r, :] * jnp.exp(m_old - m_new)
            hi, lo = cand_hi[r, :], cand_lo[r, :]
            q = q_part[r, :]
            for j, z in enumerate(zs):
                total = total + jnp.exp(z - m_new)
                picked = jnp.take_along_axis(z, lo, axis=1, mode="promise_in_bounds")
                q = jnp.where(hi == t * (tile // LANES) + j, picked, q)
            m_ref[r, :] = m_new
            l_ref[r, :] = total
            q_part[r, :] = q

    raws = (raw_a, raw_b)

    load(0, 0).wait()
    start_any(depth - 1)
    dot(0, raw_a, tile)

    def step(t, parity):
        slot = lax.rem(t, depth)
        load(t, slot).wait()
        nxt = t + depth - 1

        @pl.when(nxt < full)
        def _():
            load(nxt, lax.rem(nxt, depth)).start()

        if rest:
            @pl.when(nxt == full)
            def _():
                load_rest(full % depth).start()

        dot(slot, raws[parity], tile)
        epilogue(t - 1, raws[1 - parity], tile)

    pairs = (full - 1) // 2

    def pair(i, carry):
        step(1 + 2 * i, 1)
        step(2 + 2 * i, 0)
        return carry

    lax.fori_loop(0, pairs, pair, 0)
    last = 2 * pairs
    if last < full - 1:
        last += 1
        step(jnp.int32(last), 1)
    if rest:
        load_rest(full % depth).wait()
        dot(full % depth, raws[(last + 1) % 2], rest)
        epilogue(last, raws[last % 2], tile)
        epilogue(full, raws[(last + 1) % 2], rest)
    else:
        epilogue(last, raws[last % 2], tile)

    m_t = m_ref[...].T
    top = jnp.max(m_t, axis=0, keepdims=True)
    total = jnp.sum(l_ref[...].T * jnp.exp(m_t - top), axis=0, keepdims=True)
    sub = lax.broadcasted_iota(jnp.int32, (8, LANES), 0)
    stats = jnp.where(sub == 0, jnp.broadcast_to(top, (8, LANES)), jnp.broadcast_to(total, (8, LANES)))
    stat_send[...] = stats
    stat_recv[me] = stats

    pl.semaphore_wait(barrier, n_dev - 1)

    def stat_copy(k):
        peer = lax.rem(me + k, n_dev)
        return pltpu.make_async_remote_copy(
            src_ref=stat_send, dst_ref=stat_recv.at[me], send_sem=stat_ssem.at[k], recv_sem=stat_rsem.at[k],
            device_id=(peer,), device_id_type=MESH_ID)

    def rs_copy(k):
        peer = lax.rem(me + k, n_dev)
        return pltpu.make_async_remote_copy(
            src_ref=q_part.at[pl.ds(pl.multiple_of(peer * own_rows, 8), own_rows)], dst_ref=qrs_recv.at[k],
            send_sem=rs_ssem.at[k], recv_sem=rs_rsem.at[k], device_id=(peer,), device_id_type=MESH_ID)

    def ag_copy(k):
        peer = lax.rem(me + k, n_dev)
        return pltpu.make_async_remote_copy(
            src_ref=q_own, dst_ref=q_all.at[pl.ds(pl.multiple_of(me * own_rows, 8), own_rows)],
            send_sem=ag_ssem.at[k], recv_sem=ag_rsem.at[k], device_id=(peer,), device_id_type=MESH_ID)

    stat_copies = [stat_copy(k) for k in range(1, n_dev)]
    rs_copies = [rs_copy(k) for k in range(1, n_dev)]
    ag_copies = [ag_copy(k) for k in range(1, n_dev)]
    for c in stat_copies:
        c.start()
    for c in rs_copies:
        c.start()
    for c in rs_copies:
        c.wait()
    mine = pl.ds(pl.multiple_of(me * own_rows, 8), own_rows)
    own = q_part[mine, :]
    for k in range(1, n_dev):
        own = own + qrs_recv[k]
    q_own[...] = own
    for c in ag_copies:
        c.start()
    for c in stat_copies:
        c.wait()
    every = stat_recv[...]
    tops = every[:, 0, :]
    sums = every[:, 1, :]
    top = jnp.max(tops, axis=0, keepdims=True)
    total = jnp.sum(sums * jnp.exp(tops - top), axis=0, keepdims=True)
    logz = top + jnp.log(total)
    logz_ref[...] = jnp.broadcast_to(logz, (LANES, rows)).T
    for c in ag_copies:
        c.wait()
    q_all[mine, :] = own
    q_ref[...] = q_all[...]


def write_kernel(z_ref, logz_ref, q_ref, lp_ref, cand_lp_ref, stage, sem):
    rows, columns = z_ref.shape
    groups = rows // 8
    depth = stage.shape[0]

    def put(g):
        return pltpu.make_async_copy(stage.at[g % depth], lp_ref.at[pl.ds(8 * g, 8)], sem.at[g % depth])

    for g in range(groups):
        if g >= depth:
            put(g - depth).wait()
        r = pl.ds(8 * g, 8)
        norm = logz_ref[r, :]
        for j in range(columns // LANES):
            c = slice(j * LANES, (j + 1) * LANES)
            stage[g % depth, :, c] = z_ref[r, c] - norm
        put(g).start()
    cand_lp_ref[...] = q_ref[...] - logz_ref[...]
    for g in range(groups - depth, groups):
        put(g).wait()


def solution(mesh):
    axis_name = mesh.axis_names[0]
    n_dev = mesh.shape[axis_name]

    def per_device(hidden, ln_weight, ln_bias, emb_shard, temperature, cand_ids):
        rows, feat = hidden.shape
        columns = emb_shard.shape[0]
        cands = cand_ids.shape[1]
        full, rest = split_columns(columns, TILE)
        f32 = jnp.float32
        vmem = pl.BlockSpec(memory_space=pltpu.VMEM)
        own_rows = rows // n_dev
        z, logz, q = pl.pallas_call(
            functools.partial(head_kernel, axis_name, n_dev, TILE, full, rest),
            out_shape=(
                pltpu.VMEM((rows, columns), f32),
                pltpu.VMEM((rows, LANES), f32),
                pltpu.VMEM((rows, cands), f32),
            ),
            in_specs=[pl.BlockSpec(memory_space=pltpu.SMEM)] + [vmem] * 4 + [pl.BlockSpec(memory_space=pl.ANY)],
            out_specs=(vmem, vmem, vmem),
            scratch_shapes=[
                pltpu.VMEM((DEPTH, TILE, feat), jnp.bfloat16),
                pltpu.VMEM((rows, TILE), f32),
                pltpu.VMEM((rows, TILE), f32),
                pltpu.VMEM((rows, feat), jnp.bfloat16),
                pltpu.VMEM((rows, LANES), f32),
                pltpu.VMEM((rows, LANES), f32),
                pltpu.VMEM((rows, cands), jnp.int32),
                pltpu.VMEM((rows, cands), jnp.int32),
                pltpu.VMEM((rows, cands), f32),
                pltpu.VMEM((8, LANES), f32),
                pltpu.VMEM((n_dev, 8, LANES), f32),
                pltpu.VMEM((n_dev, own_rows, cands), f32),
                pltpu.VMEM((own_rows, cands), f32),
                pltpu.VMEM((rows, cands), f32),
                pltpu.SemaphoreType.DMA((DEPTH,)),
                pltpu.SemaphoreType.DMA((n_dev,)),
                pltpu.SemaphoreType.DMA((n_dev,)),
                pltpu.SemaphoreType.DMA((n_dev,)),
                pltpu.SemaphoreType.DMA((n_dev,)),
                pltpu.SemaphoreType.DMA((n_dev,)),
                pltpu.SemaphoreType.DMA((n_dev,)),
            ],
            compiler_params=pltpu.CompilerParams(
                collective_id=0, has_side_effects=True, vmem_limit_bytes=44 * 1024 * 1024),
            name="head",
        )(temperature.reshape(1, 1), hidden, ln_weight.reshape(1, feat), ln_bias.reshape(1, feat), cand_ids, emb_shard)
        lp = z - logz[:, :1]
        cand_lp = q - logz
        return lp, cand_lp

    return jax.shard_map(
        per_device,
        mesh=mesh,
        in_specs=(P(), P(), P(), P(axis_name, None), P(), P()),
        out_specs=(P(None, axis_name), P()),
        check_vma=False,
    )
```

```python
import functools

import jax
import jax.numpy as jnp
from jax import lax
from jax.experimental import pallas as pl
from jax.experimental.pallas import tpu as pltpu
from jax.sharding import PartitionSpec as P

MESH_ID = pl.DeviceIdType.MESH
LANES = 128
MXU = 256
TILE = 640
UNROLL = 7
DEPTH = 14
ACC_OF = (0, 1, 0, 1, 0, 1, 2)


def head_kernel(
    axis_name,
    temp_ref, x_ref, w_ref, b_ref, cand_ref, emb_ref,
    z_ref, stat_ref, q_ref,
    ebuf, raw, zbuf, normed, m_ref, l_ref, cand_hi, cand_lo, e_sem,
):
    me = lax.axis_index(axis_name)
    rows, feat = x_ref.shape
    columns = emb_ref.shape[0]
    tiles = columns // TILE
    passes = feat // MXU
    half = TILE // 2
    blocks = TILE // LANES

    def load(t, slot):
        return pltpu.make_async_copy(
            emb_ref.at[pl.ds(pl.multiple_of(t * TILE, LANES), TILE)], ebuf.at[slot], e_sem.at[slot])

    for t in range(DEPTH - 1):
        load(t, t).start()

    xf = x_ref[...].astype(jnp.float32)
    mean = jnp.mean(xf, axis=-1, keepdims=True)
    cent = xf - mean
    var = jnp.mean(cent * cent, axis=-1, keepdims=True)
    scaled = cent * lax.rsqrt(var + 1e-5)
    normed[:rows, :] = (
        scaled * w_ref[...].astype(jnp.float32)[None] + b_ref[...].astype(jnp.float32)[None]).astype(jnp.bfloat16)
    normed[rows:, :] = jnp.zeros((MXU - rows, feat), jnp.bfloat16)
    local = cand_ref[...] - me * columns
    cand_hi[...] = local >> 7
    cand_lo[...] = local & (LANES - 1)
    m_ref[...] = jnp.full_like(m_ref, -jnp.inf)
    l_ref[...] = jnp.zeros_like(l_ref)
    q_ref[...] = jnp.zeros_like(q_ref)
    raw[UNROLL - 1] = jnp.zeros_like(raw[UNROLL - 1])
    inv_t = 1.0 / jnp.full((8, LANES), temp_ref[0, 0], jnp.float32)

    def push(k):
        for q in range(2):
            pltpu.matmul_push_rhs(
                normed[:, k * MXU:(k + 1) * MXU], staging_register=k % 2, mxu_index=q, transpose=True)

    def epilogue(t, i, first):
        column = jnp.maximum(t, 0) * TILE
        base = jnp.where(first, -(1 << 26), t * blocks)
        for j in range(blocks):
            c = slice(j * LANES, (j + 1) * LANES)
            zbuf[i % 2, :, c] = raw[i, c, :].T
        for g in range(rows // 8):
            r = pl.ds(8 * g, 8)
            zs = []
            for j in range(blocks):
                z = zbuf[i % 2, r, j * LANES:(j + 1) * LANES] * inv_t
                z_ref[r, pl.ds(pl.multiple_of(column + j * LANES, LANES), LANES)] = z
                zs.append(z)
            m_old = m_ref[r, :]
            m_new = jnp.maximum(m_old, functools.reduce(jnp.maximum, zs))
            total = l_ref[r, :] * jnp.exp(m_old - m_new)
            hi, lo = cand_hi[r, :], cand_lo[r, :]
            q = q_ref[r, :]
            for j, z in enumerate(zs):
                total = total + jnp.exp(z - m_new)
                picked = jnp.take_along_axis(z, lo, axis=1, mode="promise_in_bounds")
                q = jnp.where(hi == base + j, picked, q)
            if first is not False:
                m_new = jnp.where(first, -jnp.inf, m_new)
                total = jnp.where(first, 0.0, total)
            m_ref[r, :] = m_new
            l_ref[r, :] = total
            q_ref[r, :] = q

    def body(*accs):
        accs = (accs[:3], accs[3:])

        def pop(i):
            for q in range(2):
                raw[i, q * half:(q + 1) * half, :] = pltpu.matmul_pop(accs[q][ACC_OF[i]])[:, :LANES]

        def trip(it, carry):
            for i in range(UNROLL):
                t = it * UNROLL + i
                slot = lax.rem(t, DEPTH)
                load(t, slot).wait()
                nxt = t + DEPTH - 1

                @pl.when(nxt < tiles)
                def _():
                    load(nxt, lax.rem(nxt, DEPTH)).start()

                for k in range(passes):
                    for q in range(2):
                        pltpu.matmul_acc_lhs(
                            accs[q][ACC_OF[i]],
                            ebuf[slot, q * half:(q + 1) * half, k * MXU:(k + 1) * MXU],
                            load_staged_rhs=k % 2)
                    push((k + 1) % passes)
                    if k == 1 and i > 0:
                        pop(i - 1)
                if i == 0:
                    epilogue(t - 1, UNROLL - 1, it == 0)
                else:
                    epilogue(t - 1, i - 1, False)
            pop(UNROLL - 1)
            return carry

        push(0)
        lax.fori_loop(0, tiles // UNROLL, trip, 0)
        for q in range(2):
            pltpu.matmul_acc_lhs(accs[q][2], jnp.zeros((half, MXU), jnp.bfloat16), load_staged_rhs=0)
        epilogue(jnp.int32(tiles - 1), UNROLL - 1, False)
        for q in range(2):
            raw[0, q * half:(q + 1) * half, :] = pltpu.matmul_pop(accs[q][2])[:, :LANES]

    shape = ((half, MXU), jnp.float32)
    pl.run_scoped(body, *[pltpu.ACC(0)(*shape)] * 3, *[pltpu.ACC(1)(*shape)] * 3)

    m_t = m_ref[...].T
    top = jnp.max(m_t, axis=0, keepdims=True)
    total = jnp.sum(l_ref[...].T * jnp.exp(m_t - top), axis=0, keepdims=True)
    sub = lax.broadcasted_iota(jnp.int32, (8, LANES), 0)
    stat_ref[...] = jnp.where(sub == 0, jnp.broadcast_to(top, (8, LANES)), jnp.broadcast_to(total, (8, LANES)))


def exchange_kernel(
    axis_name, n_dev,
    stat_ref, part_ref, logz_ref, q_ref,
    stat_recv, rs_recv, q_own, q_all,
    stat_ssem, stat_rsem, rs_ssem, rs_rsem, ag_ssem, ag_rsem,
):
    me = lax.axis_index(axis_name)
    rows = part_ref.shape[0]
    own_rows = rows // n_dev
    barrier = pltpu.get_barrier_semaphore()
    for k in range(1, n_dev):
        pl.semaphore_signal(barrier, inc=1, device_id=(lax.rem(me + k, n_dev),), device_id_type=MESH_ID)
    pl.semaphore_wait(barrier, n_dev - 1)

    def stat_copy(k):
        peer = lax.rem(me + k, n_dev)
        return pltpu.make_async_remote_copy(
            src_ref=stat_ref, dst_ref=stat_recv.at[k], send_sem=stat_ssem.at[k], recv_sem=stat_rsem.at[k],
            device_id=(peer,), device_id_type=MESH_ID)

    def rs_copy(k):
        peer = lax.rem(me + k, n_dev)
        return pltpu.make_async_remote_copy(
            src_ref=part_ref.at[pl.ds(pl.multiple_of(peer * own_rows, 8), own_rows)], dst_ref=rs_recv.at[k],
            send_sem=rs_ssem.at[k], recv_sem=rs_rsem.at[k], device_id=(peer,), device_id_type=MESH_ID)

    def ag_copy(k):
        peer = lax.rem(me + k, n_dev)
        return pltpu.make_async_remote_copy(
            src_ref=q_own, dst_ref=q_all.at[pl.ds(pl.multiple_of(me * own_rows, 8), own_rows)],
            send_sem=ag_ssem.at[k], recv_sem=ag_rsem.at[k], device_id=(peer,), device_id_type=MESH_ID)

    stat_copies = [stat_copy(k) for k in range(1, n_dev)]
    rs_copies = [rs_copy(k) for k in range(1, n_dev)]
    ag_copies = [ag_copy(k) for k in range(1, n_dev)]
    for c in rs_copies + stat_copies:
        c.start()
    stat_recv[0] = stat_ref[...]
    mine = pl.ds(pl.multiple_of(me * own_rows, 8), own_rows)
    own = part_ref[mine, :]
    for c in rs_copies:
        c.wait()
    for k in range(1, n_dev):
        own = own + rs_recv[k]
    q_own[...] = own
    for c in ag_copies:
        c.start()
    for c in stat_copies:
        c.wait()
    tops = stat_recv[:, 0, :]
    sums = stat_recv[:, 1, :]
    top = jnp.max(tops, axis=0, keepdims=True)
    total = jnp.sum(sums * jnp.exp(tops - top), axis=0, keepdims=True)
    logz = jnp.broadcast_to(top + jnp.log(total), (LANES, rows)).T
    logz_ref[...] = logz
    for c in ag_copies:
        c.wait()
    q_all[mine, :] = own
    q_ref[...] = q_all[...] - logz


def solution(mesh):
    axis_name = mesh.axis_names[0]
    n_dev = mesh.shape[axis_name]

    def per_device(hidden, ln_weight, ln_bias, emb_shard, temperature, cand_ids):
        rows, feat = hidden.shape
        columns = emb_shard.shape[0]
        cands = cand_ids.shape[1]
        own_rows = rows // n_dev
        f32 = jnp.float32
        vmem = pl.BlockSpec(memory_space=pltpu.VMEM)
        z, stat, part = pl.pallas_call(
            functools.partial(head_kernel, axis_name),
            out_shape=(
                pltpu.VMEM((rows, columns), f32),
                pltpu.VMEM((8, LANES), f32),
                pltpu.VMEM((rows, cands), f32),
            ),
            in_specs=[pl.BlockSpec(memory_space=pltpu.SMEM)] + [vmem] * 4 + [pl.BlockSpec(memory_space=pl.ANY)],
            out_specs=(vmem, vmem, vmem),
            scratch_shapes=[
                pltpu.VMEM((DEPTH, TILE, feat), jnp.bfloat16),
                pltpu.VMEM((UNROLL, TILE, rows), f32),
                pltpu.VMEM((2, rows, TILE), f32),
                pltpu.VMEM((MXU, feat), jnp.bfloat16),
                pltpu.VMEM((rows, LANES), f32),
                pltpu.VMEM((rows, LANES), f32),
                pltpu.VMEM((rows, cands), jnp.int32),
                pltpu.VMEM((rows, cands), jnp.int32),
                pltpu.SemaphoreType.DMA((DEPTH,)),
            ],
            compiler_params=pltpu.CompilerParams(vmem_limit_bytes=44 * 1024 * 1024),
            name="head",
        )(temperature.reshape(1, 1), hidden, ln_weight, ln_bias, cand_ids, emb_shard)
        logz, cand_lp = pl.pallas_call(
            functools.partial(exchange_kernel, axis_name, n_dev),
            out_shape=(
                pltpu.VMEM((rows, LANES), f32),
                pltpu.VMEM((rows, cands), f32),
            ),
            in_specs=[vmem, vmem],
            out_specs=(vmem, vmem),
            scratch_shapes=[
                pltpu.VMEM((n_dev, 8, LANES), f32),
                pltpu.VMEM((n_dev, own_rows, cands), f32),
                pltpu.VMEM((own_rows, cands), f32),
                pltpu.VMEM((rows, cands), f32),
            ] + [pltpu.SemaphoreType.DMA((n_dev,))] * 6,
            compiler_params=pltpu.CompilerParams(
                collective_id=0, has_side_effects=True, vmem_limit_bytes=4 * 1024 * 1024),
            name="exchange",
        )(stat, part)
        return z - logz[:, :1], cand_lp

    return jax.shard_map(
        per_device,
        mesh=mesh,
        in_specs=(P(), P(), P(), P(axis_name, None), P(), P()),
        out_specs=(P(None, axis_name), P()),
        check_vma=False,
    )
```

```python
import functools

import jax
import jax.numpy as jnp
from jax import lax
from jax.experimental import pallas as pl
from jax.experimental.pallas import tpu as pltpu
from jax.sharding import PartitionSpec as P

MESH_ID = pl.DeviceIdType.MESH
LANES = 128
MXU = 256
TILE = 640
UNROLL = 7
DEPTH = 6
ACC_OF = (0, 1, 0, 1, 0, 1, 2)


def head_kernel(
    axis_name,
    temp_ref, x_hbm, w_hbm, b_hbm, cand_hbm, emb_ref,
    z_ref, stat_ref, q_ref,
    ebuf, raw, zbuf, normed, m_ref, l_ref, cand_hi, cand_lo, x_ref, w_ref, b_ref, cand_ref, e_sem, s_sem,
):
    me = lax.axis_index(axis_name)
    rows, feat = x_hbm.shape
    columns = emb_ref.shape[0]
    tiles = columns // TILE
    passes = feat // MXU
    half = TILE // 2
    blocks = TILE // LANES

    def load(t, slot):
        return pltpu.make_async_copy(
            emb_ref.at[pl.ds(pl.multiple_of(t * TILE, LANES), TILE)], ebuf.at[slot], e_sem.at[slot])

    small = [
        pltpu.make_async_copy(src, dst, s_sem.at[i])
        for i, (src, dst) in enumerate(((x_hbm, x_ref), (w_hbm, w_ref), (b_hbm, b_ref), (cand_hbm, cand_ref)))]
    for c in small:
        c.start()
    for t in range(2):
        load(t, t).start()
    for c in small:
        c.wait()
    for t in range(2, DEPTH - 1):
        load(t, t).start()

    xf = x_ref[...].astype(jnp.float32)
    mean = jnp.mean(xf, axis=-1, keepdims=True)
    cent = xf - mean
    var = jnp.mean(cent * cent, axis=-1, keepdims=True)
    scaled = cent * lax.rsqrt(var + 1e-5)
    normed[:rows, :] = (
        scaled * w_ref[...].astype(jnp.float32)[None] + b_ref[...].astype(jnp.float32)[None]).astype(jnp.bfloat16)
    normed[rows:, :] = jnp.zeros((MXU - rows, feat), jnp.bfloat16)
    local = cand_ref[...] - me * columns
    cand_hi[...] = local >> 7
    cand_lo[...] = local & (LANES - 1)
    m_ref[...] = jnp.full_like(m_ref, -jnp.inf)
    l_ref[...] = jnp.zeros_like(l_ref)
    q_ref[...] = jnp.zeros_like(q_ref)
    raw[UNROLL - 1] = jnp.zeros_like(raw[UNROLL - 1])
    inv_t = 1.0 / jnp.full((8, LANES), temp_ref[0, 0], jnp.float32)

    def push(k):
        for q in range(2):
            pltpu.matmul_push_rhs(
                normed[:, k * MXU:(k + 1) * MXU], staging_register=k % 2, mxu_index=q, transpose=True)

    def epilogue(t, i, first):
        column = jnp.maximum(t, 0) * TILE
        base = jnp.where(first, -(1 << 26), t * blocks)
        for j in range(blocks):
            c = slice(j * LANES, (j + 1) * LANES)
            zbuf[i % 2, :, c] = raw[i, c, :].T
        for g in range(rows // 8):
            r = pl.ds(8 * g, 8)
            zs = []
            for j in range(blocks):
                z = zbuf[i % 2, r, j * LANES:(j + 1) * LANES] * inv_t
                z_ref[r, pl.ds(pl.multiple_of(column + j * LANES, LANES), LANES)] = z
                zs.append(z)
            m_old = m_ref[r, :]
            m_new = jnp.maximum(m_old, functools.reduce(jnp.maximum, zs))
            total = l_ref[r, :] * jnp.exp(m_old - m_new)
            hi, lo = cand_hi[r, :], cand_lo[r, :]
            q = q_ref[r, :]
            for j, z in enumerate(zs):
                total = total + jnp.exp(z - m_new)
                picked = jnp.take_along_axis(z, lo, axis=1, mode="promise_in_bounds")
                q = jnp.where(hi == base + j, picked, q)
            if first is not False:
                m_new = jnp.where(first, -jnp.inf, m_new)
                total = jnp.where(first, 0.0, total)
            m_ref[r, :] = m_new
            l_ref[r, :] = total
            q_ref[r, :] = q

    def body(*accs):
        accs = (accs[:3], accs[3:])

        def pop(i):
            for q in range(2):
                raw[i, q * half:(q + 1) * half, :] = pltpu.matmul_pop(accs[q][ACC_OF[i]])[:, :LANES]

        def trip(it, carry):
            for i in range(UNROLL):
                t = it * UNROLL + i
                slot = lax.rem(t, DEPTH)
                load(t, slot).wait()
                nxt = t + DEPTH - 1

                @pl.when(nxt < tiles)
                def _():
                    load(nxt, lax.rem(nxt, DEPTH)).start()

                for k in range(passes):
                    for q in range(2):
                        pltpu.matmul_acc_lhs(
                            accs[q][ACC_OF[i]],
                            ebuf[slot, q * half:(q + 1) * half, k * MXU:(k + 1) * MXU],
                            load_staged_rhs=k % 2)
                    push((k + 1) % passes)
                    if k == 1 and i > 0:
                        pop(i - 1)
                if i == 0:
                    epilogue(t - 1, UNROLL - 1, it == 0)
                else:
                    epilogue(t - 1, i - 1, False)
            pop(UNROLL - 1)
            return carry

        push(0)
        lax.fori_loop(0, tiles // UNROLL, trip, 0)
        for q in range(2):
            pltpu.matmul_acc_lhs(accs[q][2], jnp.zeros((half, MXU), jnp.bfloat16), load_staged_rhs=0)
        epilogue(jnp.int32(tiles - 1), UNROLL - 1, False)
        for q in range(2):
            raw[0, q * half:(q + 1) * half, :] = pltpu.matmul_pop(accs[q][2])[:, :LANES]

    shape = ((half, MXU), jnp.float32)
    pl.run_scoped(body, *[pltpu.ACC(0)(*shape)] * 3, *[pltpu.ACC(1)(*shape)] * 3)

    m_t = m_ref[...].T
    top = jnp.max(m_t, axis=0, keepdims=True)
    total = jnp.sum(l_ref[...].T * jnp.exp(m_t - top), axis=0, keepdims=True)
    sub = lax.broadcasted_iota(jnp.int32, (8, LANES), 0)
    stat_ref[...] = jnp.where(sub == 0, jnp.broadcast_to(top, (8, LANES)), jnp.broadcast_to(total, (8, LANES)))


def exchange_kernel(
    axis_name, n_dev,
    stat_ref, part_ref, logz_ref, q_ref,
    stat_recv, rs_recv, q_own, q_all,
    stat_ssem, stat_rsem, rs_ssem, rs_rsem, ag_ssem, ag_rsem,
):
    me = lax.axis_index(axis_name)
    rows = part_ref.shape[0]
    own_rows = rows // n_dev
    barrier = pltpu.get_barrier_semaphore()
    for k in range(1, n_dev):
        pl.semaphore_signal(barrier, inc=1, device_id=(lax.rem(me + k, n_dev),), device_id_type=MESH_ID)
    pl.semaphore_wait(barrier, n_dev - 1)

    def stat_copy(k):
        peer = lax.rem(me + k, n_dev)
        return pltpu.make_async_remote_copy(
            src_ref=stat_ref, dst_ref=stat_recv.at[k], send_sem=stat_ssem.at[k], recv_sem=stat_rsem.at[k],
            device_id=(peer,), device_id_type=MESH_ID)

    def rs_copy(k):
        peer = lax.rem(me + k, n_dev)
        return pltpu.make_async_remote_copy(
            src_ref=part_ref.at[pl.ds(pl.multiple_of(peer * own_rows, 8), own_rows)], dst_ref=rs_recv.at[k],
            send_sem=rs_ssem.at[k], recv_sem=rs_rsem.at[k], device_id=(peer,), device_id_type=MESH_ID)

    def ag_copy(k):
        peer = lax.rem(me + k, n_dev)
        return pltpu.make_async_remote_copy(
            src_ref=q_own, dst_ref=q_all.at[pl.ds(pl.multiple_of(me * own_rows, 8), own_rows)],
            send_sem=ag_ssem.at[k], recv_sem=ag_rsem.at[k], device_id=(peer,), device_id_type=MESH_ID)

    stat_copies = [stat_copy(k) for k in range(1, n_dev)]
    rs_copies = [rs_copy(k) for k in range(1, n_dev)]
    ag_copies = [ag_copy(k) for k in range(1, n_dev)]
    for c in rs_copies + stat_copies:
        c.start()
    stat_recv[0] = stat_ref[...]
    mine = pl.ds(pl.multiple_of(me * own_rows, 8), own_rows)
    own = part_ref[mine, :]
    for c in rs_copies:
        c.wait()
    for k in range(1, n_dev):
        own = own + rs_recv[k]
    q_own[...] = own
    for c in ag_copies:
        c.start()
    for c in stat_copies:
        c.wait()
    tops = stat_recv[:, 0, :]
    sums = stat_recv[:, 1, :]
    top = jnp.max(tops, axis=0, keepdims=True)
    total = jnp.sum(sums * jnp.exp(tops - top), axis=0, keepdims=True)
    logz = jnp.broadcast_to(top + jnp.log(total), (LANES, rows)).T
    logz_ref[...] = logz
    for c in ag_copies:
        c.wait()
    q_all[mine, :] = own
    q_ref[...] = q_all[...] - logz


def write_kernel(z_ref, logz_ref, q_ref, lp_ref, cand_lp_ref):
    columns = z_ref.shape[1]
    for g in range(4):
        r = slice(8 * g, 8 * g + 8)
        norm = logz_ref[r, :]
        for j in range(columns // LANES):
            c = slice(j * LANES, (j + 1) * LANES)
            lp_ref[r, c] = z_ref[r, c] - norm
    cand_lp_ref[...] = q_ref[...]


def solution(mesh):
    axis_name = mesh.axis_names[0]
    n_dev = mesh.shape[axis_name]

    def per_device(hidden, ln_weight, ln_bias, emb_shard, temperature, cand_ids):
        rows, feat = hidden.shape
        columns = emb_shard.shape[0]
        cands = cand_ids.shape[1]
        own_rows = rows // n_dev
        f32 = jnp.float32
        vmem = pl.BlockSpec(memory_space=pltpu.VMEM)
        z, stat, part = pl.pallas_call(
            functools.partial(head_kernel, axis_name),
            out_shape=(
                pltpu.VMEM((rows, columns), f32),
                pltpu.VMEM((8, LANES), f32),
                pltpu.VMEM((rows, cands), f32),
            ),
            in_specs=[pl.BlockSpec(memory_space=pltpu.SMEM)] + [pl.BlockSpec(memory_space=pl.ANY)] * 5,
            out_specs=(vmem, vmem, vmem),
            scratch_shapes=[
                pltpu.VMEM((DEPTH, TILE, feat), jnp.bfloat16),
                pltpu.VMEM((UNROLL, TILE, rows), f32),
                pltpu.VMEM((2, rows, TILE), f32),
                pltpu.VMEM((MXU, feat), jnp.bfloat16),
                pltpu.VMEM((rows, LANES), f32),
                pltpu.VMEM((rows, LANES), f32),
                pltpu.VMEM((rows, cands), jnp.int32),
                pltpu.VMEM((rows, cands), jnp.int32),
                pltpu.VMEM((rows, feat), jnp.bfloat16),
                pltpu.VMEM((feat,), jnp.bfloat16),
                pltpu.VMEM((feat,), jnp.bfloat16),
                pltpu.VMEM((rows, cands), jnp.int32),
                pltpu.SemaphoreType.DMA((DEPTH,)),
                pltpu.SemaphoreType.DMA((4,)),
            ],
            compiler_params=pltpu.CompilerParams(vmem_limit_bytes=44 * 1024 * 1024),
            name="head",
        )(temperature.reshape(1, 1), hidden, ln_weight, ln_bias, cand_ids, emb_shard)
        logz, cand_lp = pl.pallas_call(
            functools.partial(exchange_kernel, axis_name, n_dev),
            out_shape=(
                pltpu.VMEM((rows, LANES), f32),
                pltpu.VMEM((rows, cands), f32),
            ),
            in_specs=[vmem, vmem],
            out_specs=(vmem, vmem),
            scratch_shapes=[
                pltpu.VMEM((n_dev, 8, LANES), f32),
                pltpu.VMEM((n_dev, own_rows, cands), f32),
                pltpu.VMEM((own_rows, cands), f32),
                pltpu.VMEM((rows, cands), f32),
            ] + [pltpu.SemaphoreType.DMA((n_dev,))] * 6,
            compiler_params=pltpu.CompilerParams(
                collective_id=0, has_side_effects=True, vmem_limit_bytes=4 * 1024 * 1024),
            name="exchange",
        )(stat, part)
        lp, cand_out = pl.pallas_call(
            write_kernel,
            grid=(rows // 32,),
            out_shape=(
                jax.ShapeDtypeStruct((rows, columns), f32),
                jax.ShapeDtypeStruct((rows, cands), f32),
            ),
            in_specs=[pl.BlockSpec((32, columns), lambda i: (i, 0)), pl.BlockSpec((32, LANES), lambda i: (i, 0)), pl.BlockSpec((32, cands), lambda i: (i, 0))],
            out_specs=(pl.BlockSpec((32, columns), lambda i: (i, 0)), pl.BlockSpec((32, cands), lambda i: (i, 0))),
            compiler_params=pltpu.CompilerParams(vmem_limit_bytes=24 * 1024 * 1024),
            name="write",
        )(z, logz, cand_lp)
        return lp, cand_out

    return jax.shard_map(
        per_device,
        mesh=mesh,
        in_specs=(P(), P(), P(), P(axis_name, None), P(), P()),
        out_specs=(P(None, axis_name), P()),
        check_vma=False,
    )
```

```python
import functools

import jax
import jax.numpy as jnp
from jax import lax
from jax.experimental import pallas as pl
from jax.experimental.pallas import tpu as pltpu
from jax.sharding import PartitionSpec as P

MESH_ID = pl.DeviceIdType.MESH
LANES = 128
MXU = 256
TILE = 640
UNROLL = 6
DEPTH = 8
ACCS = 3


def head_kernel(
    axis_name,
    temp_ref, x_hbm, w_hbm, b_hbm, cand_hbm, emb_ref,
    z_ref, e_tail, normed, m_ref, l_ref, q_ref, cand_hi, cand_lo, inv_ref,
    ebuf, raw, zbuf, x_ref, w_ref, b_ref, cand_ref, e_sem, s_sem, tail_sem,
):
    me = lax.axis_index(axis_name)
    rows, feat = x_hbm.shape
    columns = emb_ref.shape[0]
    tiles = columns // TILE - 1
    passes = feat // MXU
    half = TILE // 2
    blocks = TILE // LANES

    def load(t, slot):
        return pltpu.make_async_copy(
            emb_ref.at[pl.ds(pl.multiple_of(t * TILE, LANES), TILE)], ebuf.at[slot], e_sem.at[slot])

    tail = pltpu.make_async_copy(emb_ref.at[pl.ds(tiles * TILE, TILE)], e_tail, tail_sem)
    small = [
        pltpu.make_async_copy(src, dst, s_sem.at[i])
        for i, (src, dst) in enumerate(((x_hbm, x_ref), (w_hbm, w_ref), (b_hbm, b_ref), (cand_hbm, cand_ref)))]
    for c in small:
        c.start()
    for t in range(2):
        load(t, t).start()
    for c in small:
        c.wait()
    for t in range(2, DEPTH - 1):
        load(t, t).start()

    xf = x_ref[...].astype(jnp.float32)
    mean = jnp.mean(xf, axis=-1, keepdims=True)
    cent = xf - mean
    var = jnp.mean(cent * cent, axis=-1, keepdims=True)
    scaled = cent * lax.rsqrt(var + 1e-5)
    normed[:rows, :] = (
        scaled * w_ref[...].astype(jnp.float32)[None] + b_ref[...].astype(jnp.float32)[None]).astype(jnp.bfloat16)
    normed[rows:, :] = jnp.zeros((MXU - rows, feat), jnp.bfloat16)
    local = cand_ref[...] - me * columns
    cand_hi[...] = local >> 7
    cand_lo[...] = local & (LANES - 1)
    m_ref[...] = jnp.full_like(m_ref, -jnp.inf)
    l_ref[...] = jnp.zeros_like(l_ref)
    q_ref[...] = jnp.zeros_like(q_ref)
    raw[UNROLL - 1] = jnp.zeros_like(raw[UNROLL - 1])
    inv_t = 1.0 / jnp.full((8, LANES), temp_ref[0, 0], jnp.float32)
    inv_ref[...] = inv_t

    def push(k):
        for q in range(2):
            pltpu.matmul_push_rhs(
                normed[:, k * MXU:(k + 1) * MXU], staging_register=k % 2, mxu_index=q, transpose=True)

    def epilogue(t, i, first):
        column = jnp.maximum(t, 0) * TILE
        base = jnp.where(first, -(1 << 26), t * blocks)
        for j in range(blocks):
            c = slice(j * LANES, (j + 1) * LANES)
            zbuf[i % 2, :, c] = raw[i, c, :].T
        for g in range(rows // 8):
            r = pl.ds(8 * g, 8)
            zs = []
            for j in range(blocks):
                z = zbuf[i % 2, r, j * LANES:(j + 1) * LANES] * inv_t
                z_ref[r, pl.ds(pl.multiple_of(column + j * LANES, LANES), LANES)] = z
                zs.append(z)
            m_old = m_ref[r, :]
            m_new = jnp.maximum(m_old, functools.reduce(jnp.maximum, zs))
            total = l_ref[r, :] * jnp.exp(m_old - m_new)
            hi, lo = cand_hi[r, :], cand_lo[r, :]
            q = q_ref[r, :]
            for j, z in enumerate(zs):
                total = total + jnp.exp(z - m_new)
                picked = jnp.take_along_axis(z, lo, axis=1, mode="promise_in_bounds")
                q = jnp.where(hi == base + j, picked, q)
            if first is not False:
                m_new = jnp.where(first, -jnp.inf, m_new)
                total = jnp.where(first, 0.0, total)
            m_ref[r, :] = m_new
            l_ref[r, :] = total
            q_ref[r, :] = q

    def body(*accs):
        accs = (accs[:ACCS], accs[ACCS:])

        def pop(i):
            for q in range(2):
                raw[i, q * half:(q + 1) * half, :] = pltpu.matmul_pop(accs[q][i % ACCS])[:, :LANES]

        def trip(it, carry):
            for i in range(UNROLL):
                t = it * UNROLL + i
                slot = lax.rem(t, DEPTH)
                load(t, slot).wait()
                nxt = t + DEPTH - 1

                @pl.when(nxt < tiles)
                def _():
                    load(nxt, lax.rem(nxt, DEPTH)).start()

                @pl.when(nxt == tiles)
                def _():
                    tail.start()

                for k in range(passes):
                    for q in range(2):
                        pltpu.matmul_acc_lhs(
                            accs[q][i % ACCS],
                            ebuf[slot, q * half:(q + 1) * half, k * MXU:(k + 1) * MXU],
                            load_staged_rhs=k % 2)
                    push((k + 1) % passes)
                    if k == 1:
                        pop((i - 1) % UNROLL)
                epilogue(t - 1, (i - 1) % UNROLL, it == 0 if i == 0 else False)
            return carry

        for i in range(ACCS):
            pop(i)
        push(0)
        lax.fori_loop(0, tiles // UNROLL, trip, 0)
        pop(UNROLL - 1)
        for q in range(2):
            pltpu.matmul_acc_lhs(accs[q][0], jnp.zeros((half, MXU), jnp.bfloat16), load_staged_rhs=0)
        epilogue(jnp.int32(tiles - 1), UNROLL - 1, False)
        pop(0)

    shape = ((half, MXU), jnp.float32)
    pl.run_scoped(body, *[pltpu.ACC(0)(*shape)] * ACCS, *[pltpu.ACC(1)(*shape)] * ACCS)
    tail.wait()


def flipped(me, mask):
    peer = me
    for bit in (1, 2, 4):
        if mask & bit:
            peer = peer + bit * (1 - 2 * lax.rem(me // bit, 2))
    return peer


def exchange_kernel(
    axis_name, n_dev, last_block,
    e_ref, normed, m_in, l_in, q_in, cand_hi, cand_lo, inv_ref,
    z_ref, logz_ref, q_ref,
    raw, zbuf, m_ref, l_ref, send, recv, q_own, q_all, stat_send, stat_recv,
    rs_sem, stat_sem, ag_sem,
):
    me = lax.axis_index(axis_name)
    rows = m_in.shape[0]
    own_rows = rows // n_dev
    blocks = TILE // LANES
    barrier = pltpu.get_barrier_semaphore()
    order = sorted(range(1, n_dev), key=lambda k: (-(k // 2).bit_count(), k))
    peers = {k: flipped(me, k) for k in order}
    for k in order:
        pl.semaphore_signal(barrier, inc=1, device_id=(peers[k],), device_id_type=MESH_ID)
    for h in range(2):
        rr = slice(h * (TILE // 2), (h + 1) * (TILE // 2))
        raw[rr, :] = lax.dot_general(
            e_ref[rr, :], normed[:rows, :], (((1,), (1,)), ((), ())), preferred_element_type=jnp.float32)
    for j in range(blocks):
        c = slice(j * LANES, (j + 1) * LANES)
        zbuf[:, c] = raw[c, :].T
    inv_t = inv_ref[...]
    for g in range(rows // 8):
        r = pl.ds(8 * g, 8)
        zs = []
        for j in range(blocks):
            c = slice(j * LANES, (j + 1) * LANES)
            z = zbuf[r, c] * inv_t
            z_ref[r, c] = z
            zs.append(z)
        m_old = m_in[r, :]
        m_new = jnp.maximum(m_old, functools.reduce(jnp.maximum, zs))
        total = l_in[r, :] * jnp.exp(m_old - m_new)
        hi, lo = cand_hi[r, :], cand_lo[r, :]
        q = q_in[r, :]
        for j, z in enumerate(zs):
            total = total + jnp.exp(z - m_new)
            picked = jnp.take_along_axis(z, lo, axis=1, mode="promise_in_bounds")
            q = jnp.where(hi == last_block + j, picked, q)
        m_ref[r, :] = m_new
        l_ref[r, :] = total
        per = own_rows // 8
        send[g // per, 8 * (g % per):8 * (g % per) + 8, :] = q
    m_t = m_ref[...].T
    top = jnp.max(m_t, axis=0, keepdims=True)
    total = jnp.sum(l_ref[...].T * jnp.exp(m_t - top), axis=0, keepdims=True)
    stat_send[0:1, :] = top
    stat_send[1:2, :] = total
    stat_recv[0] = stat_send[...]
    pl.semaphore_wait(barrier, n_dev - 1)

    def copy(k, src, dst, sems):
        return pltpu.make_async_remote_copy(
            src_ref=src, dst_ref=dst, send_sem=sems.at[0, k], recv_sem=sems.at[1, k],
            device_id=(peers[k],), device_id_type=MESH_ID)

    rs_copies = [copy(k, send.at[peers[k]], recv.at[k], rs_sem) for k in order]
    stat_copies = [copy(k, stat_send, stat_recv.at[k], stat_sem) for k in order]
    ag_copies = [copy(k, q_own, q_all.at[me], ag_sem) for k in order]
    for c in rs_copies + stat_copies:
        c.start()
    own = send[me]
    for c in reversed(rs_copies):
        c.wait_recv()
    for k in range(1, n_dev):
        own = own + recv[k]
    q_own[...] = own
    for c in ag_copies:
        c.start()
    q_all[me] = own
    for c in stat_copies:
        c.wait_recv()
    tops = stat_recv[:, 0, :]
    sums = stat_recv[:, 1, :]
    top = jnp.max(tops, axis=0, keepdims=True)
    total = jnp.sum(sums * jnp.exp(tops - top), axis=0, keepdims=True)
    logz = jnp.broadcast_to(top + jnp.log(total), (LANES, rows)).T
    logz_ref[...] = logz
    for c in rs_copies + stat_copies:
        c.wait_send()
    for c in reversed(ag_copies):
        c.wait_recv()
    for d in range(n_dev):
        r = slice(d * own_rows, (d + 1) * own_rows)
        q_ref[r, :] = q_all[d] - logz[r, :]
    for c in ag_copies:
        c.wait_send()


def write_kernel(z_ref, tail_ref, logz_ref, q_ref, lp_ref, cand_lp_ref):
    columns = z_ref.shape[1]
    for g in range(z_ref.shape[0] // 8):
        r = slice(8 * g, 8 * g + 8)
        norm = logz_ref[r, :]
        for j in range(columns // LANES):
            c = slice(j * LANES, (j + 1) * LANES)
            lp_ref[r, c] = z_ref[r, c] - norm
        for j in range(TILE // LANES):
            c = slice(j * LANES, (j + 1) * LANES)
            lp_ref[r, columns + j * LANES:columns + (j + 1) * LANES] = tail_ref[r, c] - norm
    cand_lp_ref[...] = q_ref[...]


def solution(mesh):
    axis_name = mesh.axis_names[0]
    n_dev = mesh.shape[axis_name]

    def per_device(hidden, ln_weight, ln_bias, emb_shard, temperature, cand_ids):
        rows, feat = hidden.shape
        columns = emb_shard.shape[0]
        cands = cand_ids.shape[1]
        own_rows = rows // n_dev
        f32 = jnp.float32
        vmem = pl.BlockSpec(memory_space=pltpu.VMEM)
        main = columns - TILE
        square, square_int = pltpu.VMEM((rows, LANES), f32), pltpu.VMEM((rows, cands), jnp.int32)
        z, *state = pl.pallas_call(
            functools.partial(head_kernel, axis_name),
            out_shape=(
                pltpu.VMEM((rows, main), f32), pltpu.VMEM((TILE, feat), jnp.bfloat16),
                pltpu.VMEM((MXU, feat), jnp.bfloat16), square, square, square, square_int, square_int,
                pltpu.VMEM((8, LANES), f32),
            ),
            in_specs=[pl.BlockSpec(memory_space=pltpu.SMEM)] + [pl.BlockSpec(memory_space=pl.ANY)] * 5,
            out_specs=(vmem,) * 9,
            scratch_shapes=[
                pltpu.VMEM((DEPTH, TILE, feat), jnp.bfloat16),
                pltpu.VMEM((UNROLL, TILE, rows), f32),
                pltpu.VMEM((2, rows, TILE), f32),
                pltpu.VMEM((rows, feat), jnp.bfloat16),
                pltpu.VMEM((feat,), jnp.bfloat16),
                pltpu.VMEM((feat,), jnp.bfloat16),
                pltpu.VMEM((rows, cands), jnp.int32),
                pltpu.SemaphoreType.DMA((DEPTH,)),
                pltpu.SemaphoreType.DMA((4,)),
                pltpu.SemaphoreType.DMA,
            ],
            compiler_params=pltpu.CompilerParams(vmem_limit_bytes=40 * 1024 * 1024),
            name="head",
        )(temperature.reshape(1, 1), hidden, ln_weight, ln_bias, cand_ids, emb_shard)
        z_tail, logz, q = pl.pallas_call(
            functools.partial(exchange_kernel, axis_name, n_dev, main // LANES),
            out_shape=(pltpu.VMEM((rows, TILE), f32), square, square),
            in_specs=[vmem] * 8,
            out_specs=(vmem,) * 3,
            scratch_shapes=[
                pltpu.VMEM((TILE, rows), f32),
                pltpu.VMEM((rows, TILE), f32),
                square, square,
                pltpu.VMEM((n_dev, own_rows, cands), f32),
                pltpu.VMEM((n_dev, own_rows, cands), f32),
                pltpu.VMEM((own_rows, cands), f32),
                pltpu.VMEM((n_dev, own_rows, cands), f32),
                pltpu.VMEM((2, LANES), f32),
                pltpu.VMEM((n_dev, 2, LANES), f32),
            ] + [pltpu.SemaphoreType.DMA((2, n_dev))] * 3,
            compiler_params=pltpu.CompilerParams(
                collective_id=0, has_side_effects=True, vmem_limit_bytes=8 * 1024 * 1024),
            name="exchange",
        )(*state)
        return pl.pallas_call(
            write_kernel,
            grid=(rows // 32,),
            out_shape=(
                jax.ShapeDtypeStruct((rows, columns), f32),
                jax.ShapeDtypeStruct((rows, cands), f32),
            ),
            in_specs=[pl.BlockSpec((32, n), lambda i: (i, 0)) for n in (main, TILE, LANES, cands)],
            out_specs=(pl.BlockSpec((32, columns), lambda i: (i, 0)), pl.BlockSpec((32, cands), lambda i: (i, 0))),
            compiler_params=pltpu.CompilerParams(vmem_limit_bytes=24 * 1024 * 1024),
            name="write",
        )(z, z_tail, logz, q)

    return jax.shard_map(
        per_device,
        mesh=mesh,
        in_specs=(P(), P(), P(), P(axis_name, None), P(), P()),
        out_specs=(P(None, axis_name), P()),
        check_vma=False,
    )
```

```python
import functools

import jax
import jax.numpy as jnp
from jax import lax
from jax.experimental import pallas as pl
from jax.experimental.pallas import tpu as pltpu
from jax.sharding import PartitionSpec as P

MESH_ID = pl.DeviceIdType.MESH
LANES = 128
MXU = 256
TILE = 640
UNROLL = 6
DEPTH = 8
ACCS = 3


def head_kernel(
    axis_name,
    temp_hbm, x_hbm, w_hbm, b_hbm, cand_hbm, emb_ref,
    z_ref, e_tail, normed, m_ref, l_ref, q_ref, cand_hi, cand_lo, inv_ref,
    ebuf, raw, zbuf, x_ref, w_ref, b_ref, cand_ref, temp_ref, e_sem, s_sem, tail_sem,
):
    me = lax.axis_index(axis_name)
    rows, feat = x_hbm.shape
    columns = emb_ref.shape[0]
    tiles = columns // TILE - 1
    passes = feat // MXU
    half = TILE // 2
    blocks = TILE // LANES

    def load(t, slot):
        return pltpu.make_async_copy(
            emb_ref.at[pl.ds(pl.multiple_of(t * TILE, LANES), TILE)], ebuf.at[slot], e_sem.at[slot])

    tail = pltpu.make_async_copy(emb_ref.at[pl.ds(tiles * TILE, TILE)], e_tail, tail_sem)
    small = [
        pltpu.make_async_copy(src, dst, s_sem.at[i])
        for i, (src, dst) in enumerate((
            (x_hbm, x_ref), (w_hbm, w_ref), (b_hbm, b_ref), (cand_hbm, cand_ref), (temp_hbm, temp_ref)))]
    for c in small:
        c.start()
    for t in range(2):
        load(t, t).start()
    for c in small:
        c.wait()
    for t in range(2, DEPTH - 1):
        load(t, t).start()

    xf = x_ref[...].astype(jnp.float32)
    mean = jnp.mean(xf, axis=-1, keepdims=True)
    cent = xf - mean
    var = jnp.mean(cent * cent, axis=-1, keepdims=True)
    scaled = cent * lax.rsqrt(var + 1e-5)
    normed[:rows, :] = (
        scaled * w_ref[...].astype(jnp.float32)[None] + b_ref[...].astype(jnp.float32)[None]).astype(jnp.bfloat16)
    normed[rows:, :] = jnp.zeros((MXU - rows, feat), jnp.bfloat16)
    local = cand_ref[...] - me * columns
    cand_hi[...] = local >> 7
    cand_lo[...] = local & (LANES - 1)
    m_ref[...] = jnp.full_like(m_ref, -jnp.inf)
    l_ref[...] = jnp.zeros_like(l_ref)
    q_ref[...] = jnp.zeros_like(q_ref)
    raw[UNROLL - 1] = jnp.zeros_like(raw[UNROLL - 1])
    inv_t = 1.0 / jnp.full((8, LANES), temp_ref[0, 0], jnp.float32)
    inv_ref[...] = inv_t

    def push(k):
        for q in range(2):
            pltpu.matmul_push_rhs(
                normed[:, k * MXU:(k + 1) * MXU], staging_register=k % 2, mxu_index=q, transpose=True)

    def epilogue(t, i, first):
        column = jnp.maximum(t, 0) * TILE
        base = jnp.where(first, -(1 << 26), t * blocks)
        for j in range(blocks):
            c = slice(j * LANES, (j + 1) * LANES)
            zbuf[i % 2, :, c] = raw[i, c, :].T
        for g in range(rows // 8):
            r = pl.ds(8 * g, 8)
            zs = []
            for j in range(blocks):
                z = zbuf[i % 2, r, j * LANES:(j + 1) * LANES] * inv_t
                z_ref[r, pl.ds(pl.multiple_of(column + j * LANES, LANES), LANES)] = z
                zs.append(z)
            m_old = m_ref[r, :]
            m_new = jnp.maximum(m_old, functools.reduce(jnp.maximum, zs))
            total = l_ref[r, :] * jnp.exp(m_old - m_new)
            hi, lo = cand_hi[r, :], cand_lo[r, :]
            q = q_ref[r, :]
            for j, z in enumerate(zs):
                total = total + jnp.exp(z - m_new)
                picked = jnp.take_along_axis(z, lo, axis=1, mode="promise_in_bounds")
                q = jnp.where(hi == base + j, picked, q)
            if first is not False:
                m_new = jnp.where(first, -jnp.inf, m_new)
                total = jnp.where(first, 0.0, total)
            m_ref[r, :] = m_new
            l_ref[r, :] = total
            q_ref[r, :] = q

    def body(*accs):
        accs = (accs[:ACCS], accs[ACCS:])

        def pop(i):
            for q in range(2):
                raw[i, q * half:(q + 1) * half, :] = pltpu.matmul_pop(accs[q][i % ACCS])[:, :LANES]

        def trip(it, carry):
            for i in range(UNROLL):
                t = it * UNROLL + i
                slot = lax.rem(t, DEPTH)
                load(t, slot).wait()
                nxt = t + DEPTH - 1

                @pl.when(nxt < tiles)
                def _():
                    load(nxt, lax.rem(nxt, DEPTH)).start()

                @pl.when(nxt == tiles)
                def _():
                    tail.start()

                for k in range(passes):
                    for q in range(2):
                        pltpu.matmul_acc_lhs(
                            accs[q][i % ACCS],
                            ebuf[slot, q * half:(q + 1) * half, k * MXU:(k + 1) * MXU],
                            load_staged_rhs=k % 2)
                    push((k + 1) % passes)
                    if k == 1:
                        pop((i - 1) % UNROLL)
                epilogue(t - 1, (i - 1) % UNROLL, it == 0 if i == 0 else False)
            return carry

        for i in range(ACCS):
            pop(i)
        push(0)
        lax.fori_loop(0, tiles // UNROLL, trip, 0)
        pop(UNROLL - 1)
        for q in range(2):
            pltpu.matmul_acc_lhs(accs[q][0], jnp.zeros((half, MXU), jnp.bfloat16), load_staged_rhs=0)
        epilogue(jnp.int32(tiles - 1), UNROLL - 1, False)
        pop(0)

    shape = ((half, MXU), jnp.float32)
    pl.run_scoped(body, *[pltpu.ACC(0)(*shape)] * ACCS, *[pltpu.ACC(1)(*shape)] * ACCS)
    tail.wait()


def flipped(me, mask):
    peer = me
    for bit in (1, 2, 4):
        if mask & bit:
            peer = peer + bit * (1 - 2 * lax.rem(me // bit, 2))
    return peer


def exchange_kernel(
    axis_name, n_dev, last_block,
    e_ref, normed, m_in, l_in, q_in, cand_hi, cand_lo, inv_ref,
    z_ref, logz_ref, q_ref,
    raw, zbuf, m_ref, l_ref, send, recv, q_own, q_all, stat_send, stat_recv,
    rs_sem, stat_sem, ag_sem,
):
    me = lax.axis_index(axis_name)
    rows = m_in.shape[0]
    own_rows = rows // n_dev
    blocks = TILE // LANES
    barrier = pltpu.get_barrier_semaphore()
    order = sorted(range(1, n_dev), key=lambda k: (-(k // 2).bit_count(), k))
    peers = {k: flipped(me, k) for k in order}
    for k in order:
        pl.semaphore_signal(barrier, inc=1, device_id=(peers[k],), device_id_type=MESH_ID)
    for h in range(2):
        rr = slice(h * (TILE // 2), (h + 1) * (TILE // 2))
        raw[rr, :] = lax.dot_general(
            e_ref[rr, :], normed[:rows, :], (((1,), (1,)), ((), ())), preferred_element_type=jnp.float32)
    for j in range(blocks):
        c = slice(j * LANES, (j + 1) * LANES)
        zbuf[:, c] = raw[c, :].T
    inv_t = inv_ref[...]
    for g in range(rows // 8):
        r = pl.ds(8 * g, 8)
        zs = []
        for j in range(blocks):
            c = slice(j * LANES, (j + 1) * LANES)
            z = zbuf[r, c] * inv_t
            z_ref[r, c] = z
            zs.append(z)
        m_old = m_in[r, :]
        m_new = jnp.maximum(m_old, functools.reduce(jnp.maximum, zs))
        total = l_in[r, :] * jnp.exp(m_old - m_new)
        hi, lo = cand_hi[r, :], cand_lo[r, :]
        q = q_in[r, :]
        for j, z in enumerate(zs):
            total = total + jnp.exp(z - m_new)
            picked = jnp.take_along_axis(z, lo, axis=1, mode="promise_in_bounds")
            q = jnp.where(hi == last_block + j, picked, q)
        m_ref[r, :] = m_new
        l_ref[r, :] = total
        per = own_rows // 8
        send[g // per, 8 * (g % per):8 * (g % per) + 8, :] = q
    m_t = m_ref[...].T
    top = jnp.max(m_t, axis=0, keepdims=True)
    total = jnp.sum(l_ref[...].T * jnp.exp(m_t - top), axis=0, keepdims=True)
    stat_send[0:1, :] = top
    stat_send[1:2, :] = total
    stat_recv[0] = stat_send[...]
    pl.semaphore_wait(barrier, n_dev - 1)

    def copy(k, src, dst, sems):
        return pltpu.make_async_remote_copy(
            src_ref=src, dst_ref=dst, send_sem=sems.at[0, k], recv_sem=sems.at[1, k],
            device_id=(peers[k],), device_id_type=MESH_ID)

    rs_copies = [copy(k, send.at[peers[k]], recv.at[k], rs_sem) for k in order]
    stat_copies = [copy(k, stat_send, stat_recv.at[k], stat_sem) for k in order]
    ag_copies = [copy(k, q_own, q_all.at[me], ag_sem) for k in order]
    for c in rs_copies + stat_copies:
        c.start()
    own = send[me]
    for c in reversed(rs_copies):
        c.wait_recv()
    for k in range(1, n_dev):
        own = own + recv[k]
    q_own[...] = own
    for c in ag_copies:
        c.start()
    q_all[me] = own
    for c in stat_copies:
        c.wait_recv()
    tops = stat_recv[:, 0, :]
    sums = stat_recv[:, 1, :]
    top = jnp.max(tops, axis=0, keepdims=True)
    total = jnp.sum(sums * jnp.exp(tops - top), axis=0, keepdims=True)
    logz = jnp.broadcast_to(top + jnp.log(total), (LANES, rows)).T
    logz_ref[...] = logz
    for c in rs_copies + stat_copies:
        c.wait_send()
    for c in reversed(ag_copies):
        c.wait_recv()
    for d in range(n_dev):
        r = slice(d * own_rows, (d + 1) * own_rows)
        q_ref[r, :] = q_all[d] - logz[r, :]
    for c in ag_copies:
        c.wait_send()


def write_kernel(z_ref, tail_ref, logz_ref, q_ref, lp_ref, cand_lp_ref):
    columns = z_ref.shape[1]
    for g in range(z_ref.shape[0] // 8):
        r = slice(8 * g, 8 * g + 8)
        norm = logz_ref[r, :]
        for j in range(columns // LANES):
            c = slice(j * LANES, (j + 1) * LANES)
            lp_ref[r, c] = z_ref[r, c] - norm
        for j in range(TILE // LANES):
            c = slice(j * LANES, (j + 1) * LANES)
            lp_ref[r, columns + j * LANES:columns + (j + 1) * LANES] = tail_ref[r, c] - norm
    cand_lp_ref[...] = q_ref[...]


def solution(mesh):
    axis_name = mesh.axis_names[0]
    n_dev = mesh.shape[axis_name]

    def per_device(hidden, ln_weight, ln_bias, emb_shard, temperature, cand_ids):
        rows, feat = hidden.shape
        columns = emb_shard.shape[0]
        cands = cand_ids.shape[1]
        own_rows = rows // n_dev
        f32 = jnp.float32
        vmem = pl.BlockSpec(memory_space=pltpu.VMEM)
        main = columns - TILE
        square, square_int = pltpu.VMEM((rows, LANES), f32), pltpu.VMEM((rows, cands), jnp.int32)
        z, *state = pl.pallas_call(
            functools.partial(head_kernel, axis_name),
            out_shape=(
                pltpu.VMEM((rows, main), f32), pltpu.VMEM((TILE, feat), jnp.bfloat16),
                pltpu.VMEM((MXU, feat), jnp.bfloat16), square, square, square, square_int, square_int,
                pltpu.VMEM((8, LANES), f32),
            ),
            in_specs=[pl.BlockSpec(memory_space=pl.ANY)] * 6,
            out_specs=(vmem,) * 9,
            scratch_shapes=[
                pltpu.VMEM((DEPTH, TILE, feat), jnp.bfloat16),
                pltpu.VMEM((UNROLL, TILE, rows), f32),
                pltpu.VMEM((2, rows, TILE), f32),
                pltpu.VMEM((rows, feat), jnp.bfloat16),
                pltpu.VMEM((feat,), jnp.bfloat16),
                pltpu.VMEM((feat,), jnp.bfloat16),
                pltpu.VMEM((rows, cands), jnp.int32),
                pltpu.SMEM((1, 1), f32),
                pltpu.SemaphoreType.DMA((DEPTH,)),
                pltpu.SemaphoreType.DMA((5,)),
                pltpu.SemaphoreType.DMA,
            ],
            compiler_params=pltpu.CompilerParams(vmem_limit_bytes=40 * 1024 * 1024),
            name="head",
        )(temperature.reshape(1, 1), hidden, ln_weight, ln_bias, cand_ids, emb_shard)
        z_tail, logz, q = pl.pallas_call(
            functools.partial(exchange_kernel, axis_name, n_dev, main // LANES),
            out_shape=(pltpu.VMEM((rows, TILE), f32), square, square),
            in_specs=[vmem] * 8,
            out_specs=(vmem,) * 3,
            scratch_shapes=[
                pltpu.VMEM((TILE, rows), f32),
                pltpu.VMEM((rows, TILE), f32),
                square, square,
                pltpu.VMEM((n_dev, own_rows, cands), f32),
                pltpu.VMEM((n_dev, own_rows, cands), f32),
                pltpu.VMEM((own_rows, cands), f32),
                pltpu.VMEM((n_dev, own_rows, cands), f32),
                pltpu.VMEM((2, LANES), f32),
                pltpu.VMEM((n_dev, 2, LANES), f32),
            ] + [pltpu.SemaphoreType.DMA((2, n_dev))] * 3,
            compiler_params=pltpu.CompilerParams(
                collective_id=0, has_side_effects=True, vmem_limit_bytes=8 * 1024 * 1024),
            name="exchange",
        )(*state)
        return pl.pallas_call(
            write_kernel,
            grid=(rows // 32,),
            out_shape=(
                jax.ShapeDtypeStruct((rows, columns), f32),
                jax.ShapeDtypeStruct((rows, cands), f32),
            ),
            in_specs=[pl.BlockSpec((32, n), lambda i: (i, 0)) for n in (main, TILE, LANES, cands)],
            out_specs=(pl.BlockSpec((32, columns), lambda i: (i, 0)), pl.BlockSpec((32, cands), lambda i: (i, 0))),
            compiler_params=pltpu.CompilerParams(vmem_limit_bytes=24 * 1024 * 1024),
            name="write",
        )(z, z_tail, logz, q)

    return jax.shard_map(
        per_device,
        mesh=mesh,
        in_specs=(P(), P(), P(), P(axis_name, None), P(), P()),
        out_specs=(P(None, axis_name), P()),
        check_vma=False,
    )
```

```python
import functools

import jax
import jax.numpy as jnp
from jax import lax
from jax.experimental import pallas as pl
from jax.experimental.pallas import tpu as pltpu
from jax.sharding import PartitionSpec as P

MESH_ID = pl.DeviceIdType.MESH
LANES = 128
MXU = 256
TILE = 640
UNROLL = 6
DEPTH = 8
ACCS = 3


def head_kernel(
    axis_name,
    temp_hbm, x_hbm, w_hbm, b_hbm, cand_hbm, emb_ref,
    z_ref, e_tail, normed, m_ref, l_ref, q_ref, cand_hi, cand_lo, inv_ref,
    ebuf, raw, zbuf, x_ref, w_ref, b_ref, cand_ref, temp_ref, e_sem, s_sem, tail_sem,
):
    me = lax.axis_index(axis_name)
    rows, feat = x_hbm.shape
    columns = emb_ref.shape[0]
    tiles = columns // TILE - 1
    passes = feat // MXU
    half = TILE // 2
    blocks = TILE // LANES

    def load(t, slot):
        return pltpu.make_async_copy(
            emb_ref.at[pl.ds(pl.multiple_of(t * TILE, LANES), TILE)], ebuf.at[slot], e_sem.at[slot])

    tail = pltpu.make_async_copy(emb_ref.at[pl.ds(tiles * TILE, TILE)], e_tail, tail_sem)
    small = [
        pltpu.make_async_copy(src, dst, s_sem.at[i])
        for i, (src, dst) in enumerate((
            (x_hbm, x_ref), (w_hbm, w_ref), (b_hbm, b_ref), (cand_hbm, cand_ref), (temp_hbm, temp_ref)))]
    for c in small:
        c.start()
    for t in range(3):
        load(t, t).start()
    for c in small:
        c.wait()
    for t in range(3, DEPTH - 1):
        load(t, t).start()

    xf = x_ref[...].astype(jnp.float32)
    mean = jnp.mean(xf, axis=-1, keepdims=True)
    cent = xf - mean
    var = jnp.mean(cent * cent, axis=-1, keepdims=True)
    scaled = cent * lax.rsqrt(var + 1e-5)
    normed[:rows, :] = (
        scaled * w_ref[...].astype(jnp.float32)[None] + b_ref[...].astype(jnp.float32)[None]).astype(jnp.bfloat16)
    normed[rows:, :] = jnp.zeros((MXU - rows, feat), jnp.bfloat16)
    local = cand_ref[...] - me * columns
    cand_hi[...] = local >> 7
    cand_lo[...] = local & (LANES - 1)
    m_ref[...] = jnp.full_like(m_ref, -jnp.inf)
    l_ref[...] = jnp.zeros_like(l_ref)
    q_ref[...] = jnp.zeros_like(q_ref)
    raw[UNROLL - 1] = jnp.zeros_like(raw[UNROLL - 1])
    inv_t = 1.0 / jnp.full((8, LANES), temp_ref[0, 0], jnp.float32)
    inv_ref[...] = inv_t

    def push(k):
        for q in range(2):
            pltpu.matmul_push_rhs(
                normed[:, k * MXU:(k + 1) * MXU], staging_register=k % 2, mxu_index=q, transpose=True)

    def epilogue(t, i, first):
        column = jnp.maximum(t, 0) * TILE
        base = jnp.where(first, -(1 << 26), t * blocks)
        for j in range(blocks):
            c = slice(j * LANES, (j + 1) * LANES)
            zbuf[i % 2, :, c] = raw[i, c, :].T
        for g in range(rows // 8):
            r = pl.ds(8 * g, 8)
            zs = []
            for j in range(blocks):
                z = zbuf[i % 2, r, j * LANES:(j + 1) * LANES] * inv_t
                z_ref[r, pl.ds(pl.multiple_of(column + j * LANES, LANES), LANES)] = z
                zs.append(z)
            m_old = m_ref[r, :]
            m_new = jnp.maximum(m_old, functools.reduce(jnp.maximum, zs))
            total = l_ref[r, :] * jnp.exp(m_old - m_new)
            hi, lo = cand_hi[r, :], cand_lo[r, :]
            q = q_ref[r, :]
            for j, z in enumerate(zs):
                total = total + jnp.exp(z - m_new)
                picked = jnp.take_along_axis(z, lo, axis=1, mode="promise_in_bounds")
                q = jnp.where(hi == base + j, picked, q)
            if first is not False:
                m_new = jnp.where(first, -jnp.inf, m_new)
                total = jnp.where(first, 0.0, total)
            m_ref[r, :] = m_new
            l_ref[r, :] = total
            q_ref[r, :] = q

    def body(*accs):
        accs = (accs[:ACCS], accs[ACCS:])

        def pop(i):
            for q in range(2):
                raw[i, q * half:(q + 1) * half, :] = pltpu.matmul_pop(accs[q][i % ACCS])[:, :LANES]

        def trip(it, carry):
            for i in range(UNROLL):
                t = it * UNROLL + i
                slot = lax.rem(t, DEPTH)
                load(t, slot).wait()
                nxt = t + DEPTH - 1

                @pl.when(nxt < tiles)
                def _():
                    load(nxt, lax.rem(nxt, DEPTH)).start()

                @pl.when(nxt == tiles)
                def _():
                    tail.start()

                for k in range(passes):
                    for q in range(2):
                        pltpu.matmul_acc_lhs(
                            accs[q][i % ACCS],
                            ebuf[slot, q * half:(q + 1) * half, k * MXU:(k + 1) * MXU],
                            load_staged_rhs=k % 2)
                    push((k + 1) % passes)
                    if k == 1:
                        pop((i - 1) % UNROLL)
                epilogue(t - 1, (i - 1) % UNROLL, it == 0 if i == 0 else False)
            return carry

        for i in range(ACCS):
            pop(i)
        push(0)
        lax.fori_loop(0, tiles // UNROLL, trip, 0)
        pop(UNROLL - 1)
        for q in range(2):
            pltpu.matmul_acc_lhs(accs[q][0], jnp.zeros((half, MXU), jnp.bfloat16), load_staged_rhs=0)
        epilogue(jnp.int32(tiles - 1), UNROLL - 1, False)
        pop(0)

    shape = ((half, MXU), jnp.float32)
    pl.run_scoped(body, *[pltpu.ACC(0)(*shape)] * ACCS, *[pltpu.ACC(1)(*shape)] * ACCS)
    tail.wait()


def flipped(me, mask):
    peer = me
    for bit in (1, 2, 4):
        if mask & bit:
            peer = peer + bit * (1 - 2 * lax.rem(me // bit, 2))
    return peer


def exchange_kernel(
    axis_name, n_dev, last_block,
    e_ref, normed, m_in, l_in, q_in, cand_hi, cand_lo, inv_ref,
    z_ref, logz_ref, q_ref,
    raw, zbuf, m_ref, l_ref, send, recv, q_own, q_all, stat_send, stat_recv,
    rs_sem, stat_sem, ag_sem,
):
    me = lax.axis_index(axis_name)
    rows = m_in.shape[0]
    own_rows = rows // n_dev
    blocks = TILE // LANES
    barrier = pltpu.get_barrier_semaphore()
    order = sorted(range(1, n_dev), key=lambda k: (-(k // 2).bit_count(), k))
    peers = {k: flipped(me, k) for k in order}
    for k in order:
        pl.semaphore_signal(barrier, inc=1, device_id=(peers[k],), device_id_type=MESH_ID)
    for h in range(2):
        rr = slice(h * (TILE // 2), (h + 1) * (TILE // 2))
        raw[rr, :] = lax.dot_general(
            e_ref[rr, :], normed[:rows, :], (((1,), (1,)), ((), ())), preferred_element_type=jnp.float32)
    for j in range(blocks):
        c = slice(j * LANES, (j + 1) * LANES)
        zbuf[:, c] = raw[c, :].T
    inv_t = inv_ref[...]
    for g in range(rows // 8):
        r = pl.ds(8 * g, 8)
        zs = []
        for j in range(blocks):
            c = slice(j * LANES, (j + 1) * LANES)
            z = zbuf[r, c] * inv_t
            z_ref[r, c] = z
            zs.append(z)
        m_old = m_in[r, :]
        m_new = jnp.maximum(m_old, functools.reduce(jnp.maximum, zs))
        total = l_in[r, :] * jnp.exp(m_old - m_new)
        hi, lo = cand_hi[r, :], cand_lo[r, :]
        q = q_in[r, :]
        for j, z in enumerate(zs):
            total = total + jnp.exp(z - m_new)
            picked = jnp.take_along_axis(z, lo, axis=1, mode="promise_in_bounds")
            q = jnp.where(hi == last_block + j, picked, q)
        m_ref[r, :] = m_new
        l_ref[r, :] = total
        per = own_rows // 8
        send[g // per, 8 * (g % per):8 * (g % per) + 8, :] = q
    m_t = m_ref[...].T
    top = jnp.max(m_t, axis=0, keepdims=True)
    total = jnp.sum(l_ref[...].T * jnp.exp(m_t - top), axis=0, keepdims=True)
    stat_send[0:1, :] = top
    stat_send[1:2, :] = total
    stat_recv[0] = stat_send[...]
    pl.semaphore_wait(barrier, n_dev - 1)

    def copy(k, src, dst, sems):
        return pltpu.make_async_remote_copy(
            src_ref=src, dst_ref=dst, send_sem=sems.at[0, k], recv_sem=sems.at[1, k],
            device_id=(peers[k],), device_id_type=MESH_ID)

    rs_copies = [copy(k, send.at[peers[k]], recv.at[k], rs_sem) for k in order]
    stat_copies = [copy(k, stat_send, stat_recv.at[k], stat_sem) for k in order]
    ag_copies = [copy(k, q_own, q_all.at[me], ag_sem) for k in order]
    for c in rs_copies + stat_copies:
        c.start()
    own = send[me]
    for c in reversed(rs_copies):
        c.wait_recv()
    for k in range(1, n_dev):
        own = own + recv[k]
    q_own[...] = own
    q_all[me] = own
    for c in ag_copies:
        c.start()
    for c in stat_copies:
        c.wait_recv()
    tops = stat_recv[:, 0, :]
    sums = stat_recv[:, 1, :]
    top = jnp.max(tops, axis=0, keepdims=True)
    total = jnp.sum(sums * jnp.exp(tops - top), axis=0, keepdims=True)
    logz = jnp.broadcast_to(top + jnp.log(total), (LANES, rows)).T
    logz_ref[...] = logz
    for c in rs_copies + stat_copies:
        c.wait_send()
    for c in reversed(ag_copies):
        c.wait_recv()
    for d in range(n_dev):
        r = slice(d * own_rows, (d + 1) * own_rows)
        q_ref[r, :] = q_all[d] - logz[r, :]
    for c in ag_copies:
        c.wait_send()


def write_kernel(z_ref, tail_ref, logz_ref, q_ref, lp_ref, cand_lp_ref):
    columns = z_ref.shape[1]
    for g in range(z_ref.shape[0] // 8):
        r = slice(8 * g, 8 * g + 8)
        norm = logz_ref[r, :]
        for j in range(columns // LANES):
            c = slice(j * LANES, (j + 1) * LANES)
            lp_ref[r, c] = z_ref[r, c] - norm
        for j in range(TILE // LANES):
            c = slice(j * LANES, (j + 1) * LANES)
            lp_ref[r, columns + j * LANES:columns + (j + 1) * LANES] = tail_ref[r, c] - norm
    cand_lp_ref[...] = q_ref[...]


def solution(mesh):
    axis_name = mesh.axis_names[0]
    n_dev = mesh.shape[axis_name]

    def per_device(hidden, ln_weight, ln_bias, emb_shard, temperature, cand_ids):
        rows, feat = hidden.shape
        columns = emb_shard.shape[0]
        cands = cand_ids.shape[1]
        own_rows = rows // n_dev
        f32 = jnp.float32
        vmem = pl.BlockSpec(memory_space=pltpu.VMEM)
        main = columns - TILE
        square, square_int = pltpu.VMEM((rows, LANES), f32), pltpu.VMEM((rows, cands), jnp.int32)
        z, *state = pl.pallas_call(
            functools.partial(head_kernel, axis_name),
            out_shape=(
                pltpu.VMEM((rows, main), f32), pltpu.VMEM((TILE, feat), jnp.bfloat16),
                pltpu.VMEM((MXU, feat), jnp.bfloat16), square, square, square, square_int, square_int,
                pltpu.VMEM((8, LANES), f32),
            ),
            in_specs=[pl.BlockSpec(memory_space=pl.ANY)] * 6,
            out_specs=(vmem,) * 9,
            scratch_shapes=[
                pltpu.VMEM((DEPTH, TILE, feat), jnp.bfloat16),
                pltpu.VMEM((UNROLL, TILE, rows), f32),
                pltpu.VMEM((2, rows, TILE), f32),
                pltpu.VMEM((rows, feat), jnp.bfloat16),
                pltpu.VMEM((feat,), jnp.bfloat16),
                pltpu.VMEM((feat,), jnp.bfloat16),
                pltpu.VMEM((rows, cands), jnp.int32),
                pltpu.SMEM((1, 1), f32),
                pltpu.SemaphoreType.DMA((DEPTH,)),
                pltpu.SemaphoreType.DMA((5,)),
                pltpu.SemaphoreType.DMA,
            ],
            compiler_params=pltpu.CompilerParams(vmem_limit_bytes=40 * 1024 * 1024),
            name="head",
        )(temperature.reshape(1, 1), hidden, ln_weight, ln_bias, cand_ids, emb_shard)
        z_tail, logz, q = pl.pallas_call(
            functools.partial(exchange_kernel, axis_name, n_dev, main // LANES),
            out_shape=(pltpu.VMEM((rows, TILE), f32), square, square),
            in_specs=[vmem] * 8,
            out_specs=(vmem,) * 3,
            scratch_shapes=[
                pltpu.VMEM((TILE, rows), f32),
                pltpu.VMEM((rows, TILE), f32),
                square, square,
                pltpu.VMEM((n_dev, own_rows, cands), f32),
                pltpu.VMEM((n_dev, own_rows, cands), f32),
                pltpu.VMEM((own_rows, cands), f32),
                pltpu.VMEM((n_dev, own_rows, cands), f32),
                pltpu.VMEM((2, LANES), f32),
                pltpu.VMEM((n_dev, 2, LANES), f32),
            ] + [pltpu.SemaphoreType.DMA((2, n_dev))] * 3,
            compiler_params=pltpu.CompilerParams(
                collective_id=0, has_side_effects=True, vmem_limit_bytes=8 * 1024 * 1024),
            name="exchange",
        )(*state)
        return pl.pallas_call(
            write_kernel,
            grid=(rows // 32,),
            out_shape=(
                jax.ShapeDtypeStruct((rows, columns), f32),
                jax.ShapeDtypeStruct((rows, cands), f32),
            ),
            in_specs=[pl.BlockSpec((32, n), lambda i: (i, 0)) for n in (main, TILE, LANES, cands)],
            out_specs=(pl.BlockSpec((32, columns), lambda i: (i, 0)), pl.BlockSpec((32, cands), lambda i: (i, 0))),
            compiler_params=pltpu.CompilerParams(vmem_limit_bytes=24 * 1024 * 1024),
            name="write",
        )(z, z_tail, logz, q)

    return jax.shard_map(
        per_device,
        mesh=mesh,
        in_specs=(P(), P(), P(), P(axis_name, None), P(), P()),
        out_specs=(P(None, axis_name), P()),
        check_vma=False,
    )
```

```python
import functools

import jax
import jax.numpy as jnp
from jax import lax
from jax.experimental import pallas as pl
from jax.experimental.pallas import tpu as pltpu
from jax.sharding import PartitionSpec as P

MESH_ID = pl.DeviceIdType.MESH
LANES = 128
MXU = 256
TILE = 640
UNROLL = 6
DEPTH = 8
ACCS = 3


def head_kernel(
    axis_name,
    temp_hbm, x_hbm, w_hbm, b_hbm, cand_hbm, emb_ref,
    z_ref, e_tail, normed, m_ref, l_ref, q_ref, cand_hi, cand_lo, inv_ref,
    ebuf, raw, zbuf, x_ref, w_ref, b_ref, cand_ref, temp_ref, e_sem, s_sem, tail_sem,
):
    me = lax.axis_index(axis_name)
    rows, feat = x_hbm.shape
    columns = emb_ref.shape[0]
    tiles = columns // TILE - 1
    passes = feat // MXU
    half = TILE // 2
    blocks = TILE // LANES

    def load(t, slot):
        return pltpu.make_async_copy(
            emb_ref.at[pl.ds(pl.multiple_of(t * TILE, LANES), TILE)], ebuf.at[slot], e_sem.at[slot])

    tail = pltpu.make_async_copy(emb_ref.at[pl.ds(tiles * TILE, TILE)], e_tail, tail_sem)
    small = [
        pltpu.make_async_copy(src, dst, s_sem.at[i])
        for i, (src, dst) in enumerate((
            (x_hbm, x_ref), (w_hbm, w_ref), (b_hbm, b_ref), (cand_hbm, cand_ref), (temp_hbm, temp_ref)))]
    for c in small:
        c.start()
    for t in range(3):
        load(t, t).start()
    for c in small:
        c.wait()
    for t in range(3, DEPTH - 1):
        load(t, t).start()

    xf = x_ref[...].astype(jnp.float32)
    mean = jnp.mean(xf, axis=-1, keepdims=True)
    cent = xf - mean
    var = jnp.mean(cent * cent, axis=-1, keepdims=True)
    scaled = cent * lax.rsqrt(var + 1e-5)
    normed[:rows, :] = (
        scaled * w_ref[...].astype(jnp.float32)[None] + b_ref[...].astype(jnp.float32)[None]).astype(jnp.bfloat16)
    normed[rows:, :] = jnp.zeros((MXU - rows, feat), jnp.bfloat16)
    local = cand_ref[...] - me * columns
    cand_hi[...] = local >> 7
    cand_lo[...] = local & (LANES - 1)
    m_ref[...] = jnp.full_like(m_ref, -jnp.inf)
    l_ref[...] = jnp.zeros_like(l_ref)
    q_ref[...] = jnp.zeros_like(q_ref)
    raw[UNROLL - 1] = jnp.zeros_like(raw[UNROLL - 1])
    inv_t = 1.0 / jnp.full((8, LANES), temp_ref[0, 0], jnp.float32)
    inv_ref[...] = inv_t

    def push(k):
        for q in range(2):
            pltpu.matmul_push_rhs(
                normed[:, k * MXU:(k + 1) * MXU], staging_register=k % 2, mxu_index=q, transpose=True)

    def epilogue(t, i, first):
        column = jnp.maximum(t, 0) * TILE
        base = jnp.where(first, -(1 << 26), t * blocks)
        for j in range(blocks):
            c = slice(j * LANES, (j + 1) * LANES)
            zbuf[i % 2, :, c] = raw[i, c, :].T
        for g in range(rows // 8):
            r = pl.ds(8 * g, 8)
            zs = []
            for j in range(blocks):
                z = zbuf[i % 2, r, j * LANES:(j + 1) * LANES] * inv_t
                z_ref[r, pl.ds(pl.multiple_of(column + j * LANES, LANES), LANES)] = z
                zs.append(z)
            m_old = m_ref[r, :]
            m_new = jnp.maximum(m_old, functools.reduce(jnp.maximum, zs))
            total = l_ref[r, :] * jnp.exp(m_old - m_new)
            hi, lo = cand_hi[r, :], cand_lo[r, :]
            q = q_ref[r, :]
            for j, z in enumerate(zs):
                total = total + jnp.exp(z - m_new)
                picked = jnp.take_along_axis(z, lo, axis=1, mode="promise_in_bounds")
                q = jnp.where(hi == base + j, picked, q)
            if first is not False:
                m_new = jnp.where(first, -jnp.inf, m_new)
                total = jnp.where(first, 0.0, total)
            m_ref[r, :] = m_new
            l_ref[r, :] = total
            q_ref[r, :] = q

    def body(*accs):
        accs = (accs[:ACCS], accs[ACCS:])

        def pop(i):
            for q in range(2):
                raw[i, q * half:(q + 1) * half, :] = pltpu.matmul_pop(accs[q][i % ACCS])[:, :LANES]

        def trip(it, carry):
            for i in range(UNROLL):
                t = it * UNROLL + i
                slot = lax.rem(t, DEPTH)
                load(t, slot).wait()
                nxt = t + DEPTH - 1

                @pl.when(nxt < tiles)
                def _():
                    load(nxt, lax.rem(nxt, DEPTH)).start()

                @pl.when(nxt == tiles)
                def _():
                    tail.start()

                for k in range(passes):
                    for q in range(2):
                        pltpu.matmul_acc_lhs(
                            accs[q][i % ACCS],
                            ebuf[slot, q * half:(q + 1) * half, k * MXU:(k + 1) * MXU],
                            load_staged_rhs=k % 2)
                    push((k + 1) % passes)
                    if k == 1:
                        pop((i - 1) % UNROLL)
                epilogue(t - 1, (i - 1) % UNROLL, it == 0 if i == 0 else False)
            return carry

        for i in range(ACCS):
            pop(i)
        push(0)
        lax.fori_loop(0, tiles // UNROLL, trip, 0)
        pop(UNROLL - 1)
        for q in range(2):
            pltpu.matmul_acc_lhs(accs[q][0], jnp.zeros((half, MXU), jnp.bfloat16), load_staged_rhs=0)
        epilogue(jnp.int32(tiles - 1), UNROLL - 1, False)
        pop(0)

    shape = ((half, MXU), jnp.float32)
    pl.run_scoped(body, *[pltpu.ACC(0)(*shape)] * ACCS, *[pltpu.ACC(1)(*shape)] * ACCS)
    tail.wait()


def flipped(me, mask):
    peer = me
    for bit in (1, 2, 4):
        if mask & bit:
            peer = peer + bit * (1 - 2 * lax.rem(me // bit, 2))
    return peer


def exchange_kernel(
    axis_name, n_dev, last_block,
    e_ref, normed, m_in, l_in, q_in, cand_hi, cand_lo, inv_ref,
    z_ref, logz_ref, q_ref,
    raw, zbuf, m_ref, l_ref, send, recv, q_own, q_all, stat_send, stat_recv,
    rs_sem, stat_sem, ag_sem,
):
    me = lax.axis_index(axis_name)
    rows = m_in.shape[0]
    own_rows = rows // n_dev
    blocks = TILE // LANES
    barrier = pltpu.get_barrier_semaphore()
    order = sorted(range(1, n_dev), key=lambda k: (-(k // 2).bit_count(), k))
    peers = {k: flipped(me, k) for k in order}
    for k in order:
        pl.semaphore_signal(barrier, inc=1, device_id=(peers[k],), device_id_type=MESH_ID)
    for h in range(2):
        rr = slice(h * (TILE // 2), (h + 1) * (TILE // 2))
        raw[rr, :] = lax.dot_general(
            e_ref[rr, :], normed[:rows, :], (((1,), (1,)), ((), ())), preferred_element_type=jnp.float32)
    for j in range(blocks):
        c = slice(j * LANES, (j + 1) * LANES)
        zbuf[:, c] = raw[c, :].T
    inv_t = inv_ref[...]
    for g in range(rows // 8):
        r = pl.ds(8 * g, 8)
        zs = []
        for j in range(blocks):
            c = slice(j * LANES, (j + 1) * LANES)
            z = zbuf[r, c] * inv_t
            z_ref[r, c] = z
            zs.append(z)
        m_old = m_in[r, :]
        m_new = jnp.maximum(m_old, functools.reduce(jnp.maximum, zs))
        total = l_in[r, :] * jnp.exp(m_old - m_new)
        hi, lo = cand_hi[r, :], cand_lo[r, :]
        q = q_in[r, :]
        for j, z in enumerate(zs):
            total = total + jnp.exp(z - m_new)
            picked = jnp.take_along_axis(z, lo, axis=1, mode="promise_in_bounds")
            q = jnp.where(hi == last_block + j, picked, q)
        m_ref[r, :] = m_new
        l_ref[r, :] = total
        per = own_rows // 8
        send[g // per, 8 * (g % per):8 * (g % per) + 8, :] = q
    m_t = m_ref[...].T
    top = jnp.max(m_t, axis=0, keepdims=True)
    total = jnp.sum(l_ref[...].T * jnp.exp(m_t - top), axis=0, keepdims=True)
    stat_send[0:1, :] = top
    stat_send[1:2, :] = total
    stat_recv[0] = stat_send[...]
    pl.semaphore_wait(barrier, n_dev - 1)

    def copy(k, src, dst, sems):
        return pltpu.make_async_remote_copy(
            src_ref=src, dst_ref=dst, send_sem=sems.at[0, k], recv_sem=sems.at[1, k],
            device_id=(peers[k],), device_id_type=MESH_ID)

    rs_copies = [copy(k, send.at[peers[k]], recv.at[k], rs_sem) for k in order]
    stat_copies = [copy(k, stat_send, stat_recv.at[k], stat_sem) for k in order]
    ag_copies = [copy(k, q_own, q_all.at[me], ag_sem) for k in order]
    for c in rs_copies + stat_copies:
        c.start()
    own = send[me]
    for c in reversed(rs_copies):
        c.wait_recv()
    for k in range(1, n_dev):
        own = own + recv[k]
    q_own[...] = own
    q_all[me] = own
    for c in ag_copies:
        c.start()
    for c in stat_copies:
        c.wait_recv()
    tops = stat_recv[:, 0, :]
    sums = stat_recv[:, 1, :]
    top = jnp.max(tops, axis=0, keepdims=True)
    total = jnp.sum(sums * jnp.exp(tops - top), axis=0, keepdims=True)
    logz = jnp.broadcast_to(top + jnp.log(total), (LANES, rows)).T
    logz_ref[...] = logz
    for c in rs_copies + stat_copies:
        c.wait_send()
    for c in reversed(ag_copies):
        c.wait_recv()
    for d in range(n_dev):
        r = slice(d * own_rows, (d + 1) * own_rows)
        q_ref[r, :] = q_all[d] - logz[r, :]
    for c in ag_copies:
        c.wait_send()


def write_kernel(z_ref, tail_ref, logz_ref, q_ref, lp_ref, cand_lp_ref):
    columns = z_ref.shape[1]
    for g in range(z_ref.shape[0] // 8):
        r = slice(8 * g, 8 * g + 8)
        norm = logz_ref[r, :]
        for j in range(columns // LANES):
            c = slice(j * LANES, (j + 1) * LANES)
            lp_ref[r, c] = z_ref[r, c] - norm
        for j in range(TILE // LANES):
            c = slice(j * LANES, (j + 1) * LANES)
            lp_ref[r, columns + j * LANES:columns + (j + 1) * LANES] = tail_ref[r, c] - norm

    @pl.when(pl.program_id(0) == 0)
    def _():
        cand_lp_ref[...] = q_ref[...]


def solution(mesh):
    axis_name = mesh.axis_names[0]
    n_dev = mesh.shape[axis_name]

    def per_device(hidden, ln_weight, ln_bias, emb_shard, temperature, cand_ids):
        rows, feat = hidden.shape
        columns = emb_shard.shape[0]
        cands = cand_ids.shape[1]
        own_rows = rows // n_dev
        f32 = jnp.float32
        vmem = pl.BlockSpec(memory_space=pltpu.VMEM)
        main = columns - TILE
        square, square_int = pltpu.VMEM((rows, LANES), f32), pltpu.VMEM((rows, cands), jnp.int32)
        z, *state = pl.pallas_call(
            functools.partial(head_kernel, axis_name),
            out_shape=(
                pltpu.VMEM((rows, main), f32), pltpu.VMEM((TILE, feat), jnp.bfloat16),
                pltpu.VMEM((MXU, feat), jnp.bfloat16), square, square, square, square_int, square_int,
                pltpu.VMEM((8, LANES), f32),
            ),
            in_specs=[pl.BlockSpec(memory_space=pl.ANY)] * 6,
            out_specs=(vmem,) * 9,
            scratch_shapes=[
                pltpu.VMEM((DEPTH, TILE, feat), jnp.bfloat16),
                pltpu.VMEM((UNROLL, TILE, rows), f32),
                pltpu.VMEM((2, rows, TILE), f32),
                pltpu.VMEM((rows, feat), jnp.bfloat16),
                pltpu.VMEM((feat,), jnp.bfloat16),
                pltpu.VMEM((feat,), jnp.bfloat16),
                pltpu.VMEM((rows, cands), jnp.int32),
                pltpu.SMEM((1, 1), f32),
                pltpu.SemaphoreType.DMA((DEPTH,)),
                pltpu.SemaphoreType.DMA((5,)),
                pltpu.SemaphoreType.DMA,
            ],
            compiler_params=pltpu.CompilerParams(vmem_limit_bytes=40 * 1024 * 1024),
            name="head",
        )(temperature.reshape(1, 1), hidden, ln_weight, ln_bias, cand_ids, emb_shard)
        z_tail, logz, q = pl.pallas_call(
            functools.partial(exchange_kernel, axis_name, n_dev, main // LANES),
            out_shape=(pltpu.VMEM((rows, TILE), f32), square, square),
            in_specs=[vmem] * 8,
            out_specs=(vmem,) * 3,
            scratch_shapes=[
                pltpu.VMEM((TILE, rows), f32),
                pltpu.VMEM((rows, TILE), f32),
                square, square,
                pltpu.VMEM((n_dev, own_rows, cands), f32),
                pltpu.VMEM((n_dev, own_rows, cands), f32),
                pltpu.VMEM((own_rows, cands), f32),
                pltpu.VMEM((n_dev, own_rows, cands), f32),
                pltpu.VMEM((2, LANES), f32),
                pltpu.VMEM((n_dev, 2, LANES), f32),
            ] + [pltpu.SemaphoreType.DMA((2, n_dev))] * 3,
            compiler_params=pltpu.CompilerParams(
                collective_id=0, has_side_effects=True, vmem_limit_bytes=8 * 1024 * 1024),
            name="exchange",
        )(*state)
        return pl.pallas_call(
            write_kernel,
            grid=(rows // 32,),
            out_shape=(
                jax.ShapeDtypeStruct((rows, columns), f32),
                jax.ShapeDtypeStruct((rows, cands), f32),
            ),
            in_specs=[pl.BlockSpec((32, n), lambda i: (i, 0)) for n in (main, TILE, LANES)] + [
                pl.BlockSpec((rows, cands), lambda i: (0, 0))],
            out_specs=(pl.BlockSpec((32, columns), lambda i: (i, 0)), pl.BlockSpec((rows, cands), lambda i: (0, 0))),
            compiler_params=pltpu.CompilerParams(vmem_limit_bytes=24 * 1024 * 1024),
            name="write",
        )(z, z_tail, logz, q)

    return jax.shard_map(
        per_device,
        mesh=mesh,
        in_specs=(P(), P(), P(), P(axis_name, None), P(), P()),
        out_specs=(P(None, axis_name), P()),
        check_vma=False,
    )
```

```python
import functools

import jax
import jax.numpy as jnp
from jax import lax
from jax.experimental import pallas as pl
from jax.experimental.pallas import tpu as pltpu
from jax.sharding import PartitionSpec as P

MESH_ID = pl.DeviceIdType.MESH
LANES = 128
MXU = 256
TILE = 640
UNROLL = 6
DEPTH = 8
ACCS = 3


def head_kernel(
    axis_name,
    temp_hbm, x_hbm, w_hbm, b_hbm, cand_hbm, emb_ref,
    z_ref, e_tail, normed, m_ref, l_ref, q_ref, cand_hi, cand_lo, inv_ref,
    ebuf, raw, zbuf, x_ref, w_ref, b_ref, cand_ref, temp_ref, e_sem, s_sem, tail_sem,
):
    me = lax.axis_index(axis_name)
    rows, feat = x_hbm.shape
    columns = emb_ref.shape[0]
    tiles = columns // TILE - 1
    passes = feat // MXU
    half = TILE // 2
    blocks = TILE // LANES

    def load(t, slot):
        return pltpu.make_async_copy(
            emb_ref.at[pl.ds(pl.multiple_of(t * TILE, LANES), TILE)], ebuf.at[slot], e_sem.at[slot])

    tail = pltpu.make_async_copy(emb_ref.at[pl.ds(tiles * TILE, TILE)], e_tail, tail_sem)
    small = [
        pltpu.make_async_copy(src, dst, s_sem.at[i])
        for i, (src, dst) in enumerate((
            (x_hbm, x_ref), (w_hbm, w_ref), (b_hbm, b_ref), (cand_hbm, cand_ref), (temp_hbm, temp_ref)))]
    for c in small:
        c.start()
    for t in range(4):
        load(t, t).start()
    for c in small:
        c.wait()
    for t in range(4, DEPTH - 1):
        load(t, t).start()

    xf = x_ref[...].astype(jnp.float32)
    mean = jnp.mean(xf, axis=-1, keepdims=True)
    cent = xf - mean
    var = jnp.mean(cent * cent, axis=-1, keepdims=True)
    scaled = cent * lax.rsqrt(var + 1e-5)
    normed[:rows, :] = (
        scaled * w_ref[...].astype(jnp.float32)[None] + b_ref[...].astype(jnp.float32)[None]).astype(jnp.bfloat16)
    normed[rows:, :] = jnp.zeros((MXU - rows, feat), jnp.bfloat16)
    local = cand_ref[...] - me * columns
    cand_hi[...] = local >> 7
    cand_lo[...] = local & (LANES - 1)
    m_ref[...] = jnp.full_like(m_ref, -jnp.inf)
    l_ref[...] = jnp.zeros_like(l_ref)
    q_ref[...] = jnp.zeros_like(q_ref)
    raw[UNROLL - 1] = jnp.zeros_like(raw[UNROLL - 1])
    inv_t = 1.0 / jnp.full((8, LANES), temp_ref[0, 0], jnp.float32)
    inv_ref[...] = inv_t

    def push(k):
        for q in range(2):
            pltpu.matmul_push_rhs(
                normed[:, k * MXU:(k + 1) * MXU], staging_register=k % 2, mxu_index=q, transpose=True)

    def epilogue(t, i, first):
        column = jnp.maximum(t, 0) * TILE
        base = jnp.where(first, -(1 << 26), t * blocks)
        for j in range(blocks):
            c = slice(j * LANES, (j + 1) * LANES)
            zbuf[i % 2, :, c] = raw[i, c, :].T
        for g in range(rows // 8):
            r = pl.ds(8 * g, 8)
            zs = []
            for j in range(blocks):
                z = zbuf[i % 2, r, j * LANES:(j + 1) * LANES] * inv_t
                z_ref[r, pl.ds(pl.multiple_of(column + j * LANES, LANES), LANES)] = z
                zs.append(z)
            m_old = m_ref[r, :]
            m_new = jnp.maximum(m_old, functools.reduce(jnp.maximum, zs))
            total = l_ref[r, :] * jnp.exp(m_old - m_new)
            hi, lo = cand_hi[r, :], cand_lo[r, :]
            q = q_ref[r, :]
            for j, z in enumerate(zs):
                total = total + jnp.exp(z - m_new)
                picked = jnp.take_along_axis(z, lo, axis=1, mode="promise_in_bounds")
                q = jnp.where(hi == base + j, picked, q)
            if first is not False:
                m_new = jnp.where(first, -jnp.inf, m_new)
                total = jnp.where(first, 0.0, total)
            m_ref[r, :] = m_new
            l_ref[r, :] = total
            q_ref[r, :] = q

    def body(*accs):
        accs = (accs[:ACCS], accs[ACCS:])

        def pop(i):
            for q in range(2):
                raw[i, q * half:(q + 1) * half, :] = pltpu.matmul_pop(accs[q][i % ACCS])[:, :LANES]

        def trip(it, carry):
            for i in range(UNROLL):
                t = it * UNROLL + i
                slot = lax.rem(t, DEPTH)
                load(t, slot).wait()
                nxt = t + DEPTH - 1

                @pl.when(nxt < tiles)
                def _():
                    load(nxt, lax.rem(nxt, DEPTH)).start()

                @pl.when(nxt == tiles)
                def _():
                    tail.start()

                for k in range(passes):
                    for q in range(2):
                        pltpu.matmul_acc_lhs(
                            accs[q][i % ACCS],
                            ebuf[slot, q * half:(q + 1) * half, k * MXU:(k + 1) * MXU],
                            load_staged_rhs=k % 2)
                    push((k + 1) % passes)
                    if k == 1:
                        pop((i - 1) % UNROLL)
                epilogue(t - 1, (i - 1) % UNROLL, it == 0 if i == 0 else False)
            return carry

        for i in range(ACCS):
            pop(i)
        push(0)
        lax.fori_loop(0, tiles // UNROLL, trip, 0)
        pop(UNROLL - 1)
        for q in range(2):
            pltpu.matmul_acc_lhs(accs[q][0], jnp.zeros((half, MXU), jnp.bfloat16), load_staged_rhs=0)
        epilogue(jnp.int32(tiles - 1), UNROLL - 1, False)
        pop(0)

    shape = ((half, MXU), jnp.float32)
    pl.run_scoped(body, *[pltpu.ACC(0)(*shape)] * ACCS, *[pltpu.ACC(1)(*shape)] * ACCS)
    tail.wait()


def flipped(me, mask):
    peer = me
    for bit in (1, 2, 4):
        if mask & bit:
            peer = peer + bit * (1 - 2 * lax.rem(me // bit, 2))
    return peer


def exchange_kernel(
    axis_name, n_dev, last_block,
    e_ref, normed, m_in, l_in, q_in, cand_hi, cand_lo, inv_ref,
    z_ref, logz_ref, q_ref,
    raw, zbuf, m_ref, l_ref, send, recv, q_own, q_all, stat_send, stat_recv,
    rs_sem, stat_sem, ag_sem,
):
    me = lax.axis_index(axis_name)
    rows = m_in.shape[0]
    own_rows = rows // n_dev
    blocks = TILE // LANES
    barrier = pltpu.get_barrier_semaphore()
    order = sorted(range(1, n_dev), key=lambda k: (-(k // 2).bit_count(), k))
    peers = {k: flipped(me, k) for k in order}
    for k in order:
        pl.semaphore_signal(barrier, inc=1, device_id=(peers[k],), device_id_type=MESH_ID)
    for h in range(2):
        rr = slice(h * (TILE // 2), (h + 1) * (TILE // 2))
        raw[rr, :] = lax.dot_general(
            e_ref[rr, :], normed[:rows, :], (((1,), (1,)), ((), ())), preferred_element_type=jnp.float32)
    for j in range(blocks):
        c = slice(j * LANES, (j + 1) * LANES)
        zbuf[:, c] = raw[c, :].T
    inv_t = inv_ref[...]
    for g in range(rows // 8):
        r = pl.ds(8 * g, 8)
        zs = []
        for j in range(blocks):
            c = slice(j * LANES, (j + 1) * LANES)
            z = zbuf[r, c] * inv_t
            z_ref[r, c] = z
            zs.append(z)
        m_old = m_in[r, :]
        m_new = jnp.maximum(m_old, functools.reduce(jnp.maximum, zs))
        total = l_in[r, :] * jnp.exp(m_old - m_new)
        hi, lo = cand_hi[r, :], cand_lo[r, :]
        q = q_in[r, :]
        for j, z in enumerate(zs):
            total = total + jnp.exp(z - m_new)
            picked = jnp.take_along_axis(z, lo, axis=1, mode="promise_in_bounds")
            q = jnp.where(hi == last_block + j, picked, q)
        m_ref[r, :] = m_new
        l_ref[r, :] = total
        per = own_rows // 8
        send[g // per, 8 * (g % per):8 * (g % per) + 8, :] = q
    m_t = m_ref[...].T
    top = jnp.max(m_t, axis=0, keepdims=True)
    total = jnp.sum(l_ref[...].T * jnp.exp(m_t - top), axis=0, keepdims=True)
    stat_send[0:1, :] = top
    stat_send[1:2, :] = total
    stat_recv[0] = stat_send[...]
    pl.semaphore_wait(barrier, n_dev - 1)

    def copy(k, src, dst, sems):
        return pltpu.make_async_remote_copy(
            src_ref=src, dst_ref=dst, send_sem=sems.at[0, k], recv_sem=sems.at[1, k],
            device_id=(peers[k],), device_id_type=MESH_ID)

    rs_copies = [copy(k, send.at[peers[k]], recv.at[k], rs_sem) for k in order]
    stat_copies = [copy(k, stat_send, stat_recv.at[k], stat_sem) for k in order]
    ag_copies = [copy(k, q_own, q_all.at[me], ag_sem) for k in order]
    for c in rs_copies + stat_copies:
        c.start()
    own = send[me]
    for c in reversed(rs_copies):
        c.wait_recv()
    for k in range(1, n_dev):
        own = own + recv[k]
    q_own[...] = own
    q_all[me] = own
    for c in ag_copies:
        c.start()
    for c in stat_copies:
        c.wait_recv()
    tops = stat_recv[:, 0, :]
    sums = stat_recv[:, 1, :]
    top = jnp.max(tops, axis=0, keepdims=True)
    total = jnp.sum(sums * jnp.exp(tops - top), axis=0, keepdims=True)
    logz = jnp.broadcast_to(top + jnp.log(total), (LANES, rows)).T
    logz_ref[...] = logz
    for c in rs_copies + stat_copies:
        c.wait_send()
    for c in reversed(ag_copies):
        c.wait_recv()
    for d in range(n_dev):
        r = slice(d * own_rows, (d + 1) * own_rows)
        q_ref[r, :] = q_all[d] - logz[r, :]
    for c in ag_copies:
        c.wait_send()


def write_kernel(z_ref, tail_ref, logz_ref, q_ref, lp_ref, cand_lp_ref):
    columns = z_ref.shape[1]
    for g in range(z_ref.shape[0] // 8):
        r = slice(8 * g, 8 * g + 8)
        norm = logz_ref[r, :]
        for j in range(columns // LANES):
            c = slice(j * LANES, (j + 1) * LANES)
            lp_ref[r, c] = z_ref[r, c] - norm
        for j in range(TILE // LANES):
            c = slice(j * LANES, (j + 1) * LANES)
            lp_ref[r, columns + j * LANES:columns + (j + 1) * LANES] = tail_ref[r, c] - norm

    @pl.when(pl.program_id(0) == 0)
    def _():
        cand_lp_ref[...] = q_ref[...]


def solution(mesh):
    axis_name = mesh.axis_names[0]
    n_dev = mesh.shape[axis_name]

    def per_device(hidden, ln_weight, ln_bias, emb_shard, temperature, cand_ids):
        rows, feat = hidden.shape
        columns = emb_shard.shape[0]
        cands = cand_ids.shape[1]
        own_rows = rows // n_dev
        f32 = jnp.float32
        vmem = pl.BlockSpec(memory_space=pltpu.VMEM)
        main = columns - TILE
        square, square_int = pltpu.VMEM((rows, LANES), f32), pltpu.VMEM((rows, cands), jnp.int32)
        z, *state = pl.pallas_call(
            functools.partial(head_kernel, axis_name),
            out_shape=(
                pltpu.VMEM((rows, main), f32), pltpu.VMEM((TILE, feat), jnp.bfloat16),
                pltpu.VMEM((MXU, feat), jnp.bfloat16), square, square, square, square_int, square_int,
                pltpu.VMEM((8, LANES), f32),
            ),
            in_specs=[pl.BlockSpec(memory_space=pl.ANY)] * 6,
            out_specs=(vmem,) * 9,
            scratch_shapes=[
                pltpu.VMEM((DEPTH, TILE, feat), jnp.bfloat16),
                pltpu.VMEM((UNROLL, TILE, rows), f32),
                pltpu.VMEM((2, rows, TILE), f32),
                pltpu.VMEM((rows, feat), jnp.bfloat16),
                pltpu.VMEM((feat,), jnp.bfloat16),
                pltpu.VMEM((feat,), jnp.bfloat16),
                pltpu.VMEM((rows, cands), jnp.int32),
                pltpu.SMEM((1, 1), f32),
                pltpu.SemaphoreType.DMA((DEPTH,)),
                pltpu.SemaphoreType.DMA((5,)),
                pltpu.SemaphoreType.DMA,
            ],
            compiler_params=pltpu.CompilerParams(vmem_limit_bytes=40 * 1024 * 1024),
            name="head",
        )(temperature.reshape(1, 1), hidden, ln_weight, ln_bias, cand_ids, emb_shard)
        z_tail, logz, q = pl.pallas_call(
            functools.partial(exchange_kernel, axis_name, n_dev, main // LANES),
            out_shape=(pltpu.VMEM((rows, TILE), f32), square, square),
            in_specs=[vmem] * 8,
            out_specs=(vmem,) * 3,
            scratch_shapes=[
                pltpu.VMEM((TILE, rows), f32),
                pltpu.VMEM((rows, TILE), f32),
                square, square,
                pltpu.VMEM((n_dev, own_rows, cands), f32),
                pltpu.VMEM((n_dev, own_rows, cands), f32),
                pltpu.VMEM((own_rows, cands), f32),
                pltpu.VMEM((n_dev, own_rows, cands), f32),
                pltpu.VMEM((2, LANES), f32),
                pltpu.VMEM((n_dev, 2, LANES), f32),
            ] + [pltpu.SemaphoreType.DMA((2, n_dev))] * 3,
            compiler_params=pltpu.CompilerParams(
                collective_id=0, has_side_effects=True, vmem_limit_bytes=8 * 1024 * 1024),
            name="exchange",
        )(*state)
        return pl.pallas_call(
            write_kernel,
            grid=(rows // 32,),
            out_shape=(
                jax.ShapeDtypeStruct((rows, columns), f32),
                jax.ShapeDtypeStruct((rows, cands), f32),
            ),
            in_specs=[pl.BlockSpec((32, n), lambda i: (i, 0)) for n in (main, TILE, LANES)] + [
                pl.BlockSpec((rows, cands), lambda i: (0, 0))],
            out_specs=(pl.BlockSpec((32, columns), lambda i: (i, 0)), pl.BlockSpec((rows, cands), lambda i: (0, 0))),
            compiler_params=pltpu.CompilerParams(vmem_limit_bytes=24 * 1024 * 1024),
            name="write",
        )(z, z_tail, logz, q)

    return jax.shard_map(
        per_device,
        mesh=mesh,
        in_specs=(P(), P(), P(), P(axis_name, None), P(), P()),
        out_specs=(P(None, axis_name), P()),
        check_vma=False,
    )
```
